128 devices in a mesh: dp: 32 (over y, z, core), mp: 4 (over x).
Axes of the slice: x: 4, y: 4, z: 4, core: 2. Of those that a mesh axis runs over, the one named last changes fastest.
Arguments:
- table: float32 [262144, 512], P('dp', 'mp'), may hold values from -6 to 6
- first_moment: float32 [262144, 512], P('dp', 'mp'), may hold values from -1.8 to 1.8
- second_moment: float32 [262144, 512], P('dp', 'mp'), may hold values from 0.01 to 1
- grads: bfloat16 [65536, 512], P('dp', 'mp'), may hold values from -108 to 108
- ids: int32 [65536], P('dp'), may hold values from 0 to 262143, as said below
Outputs:
- new_table: float32 [262144, 512], P('dp', 'mp')
- new_first: float32 [262144, 512], P('dp', 'mp')
- new_second: float32 [262144, 512], P('dp', 'mp')
The draws below stay inside these ranges and needn't reach their ends.
Inputs may be any that keep to these rules, and one draw needn't show every extreme that they name: `ids`: the positions of one device name at most 256 positions' worth of rows of any one owner (rows k * 8192 to (k + 1) * 8192 - 1) and at most 64 distinct rows of one owner; in every draw one owner reaches both bounds on every device.
All inputs are finite; a program needn't handle non-finite values.
Results may differ from the reference program's by a relative error of at most 0.0003.
Values may be sent and summed in bfloat16 or wider, within the bound.
A program may use at most 64 MiB of HBM per device.

```python
import math
import jax
import jax.numpy as jnp

D = 512
ROWS_DEV = 8192
TOK_DEV = 2048
TOKENS = 65536
ROWS = 262144
N_DP = 32


def draw_grads(key, part):
    keys = jax.random.split(jax.random.fold_in(key, 11), 3)
    place = jnp.arange(TOKENS, dtype=jnp.float32)
    rising = 1.0 + 2.0 * place / (TOKENS - 1)
    noise = jnp.clip(jax.random.normal(keys[0], (TOKENS, D), jnp.float32), -4.0, 4.0)
    row_scale = jnp.exp(jax.random.uniform(keys[1], (TOKENS,), jnp.float32, math.log(0.3), math.log(3.0)))
    col_scale = jnp.exp(jax.random.uniform(keys[2], (D,), jnp.float32, math.log(0.3), math.log(3.0)))
    values = noise * (row_scale * rising)[:, None] * col_scale[None, :]
    return values.astype(jnp.bfloat16)


def draw_ids(key, part):
    keys = jax.random.split(jax.random.fold_in(key, 23), 7)
    room = TOK_DEV // N_DP
    most = 4 * room
    spread = ROWS_DEV // room
    owners = jnp.arange(N_DP, dtype=jnp.int32)
    hottest = jax.random.randint(keys[0], (), 0, N_DP, dtype=jnp.int32)
    jitter = jax.random.randint(keys[1], (N_DP, N_DP), 2, 4, dtype=jnp.int32)
    weight = (N_DP - 1 + 2 * owners)[None, :] * jitter
    is_hot = owners[None, :] == hottest
    weight = jnp.where(is_hot, 0, weight)
    spare = TOK_DEV - most
    counts = spare * weight // jnp.sum(weight, axis=1, keepdims=True)
    leftover = spare - jnp.sum(counts, axis=1, keepdims=True)
    ranking = jax.vmap(lambda k: jax.random.permutation(k, N_DP))(jax.random.split(keys[2], N_DP)).astype(jnp.int32)
    hot_rank = jnp.sum(jnp.where(is_hot, ranking, 0), axis=1, keepdims=True)
    adjusted = ranking - (ranking > hot_rank).astype(jnp.int32)
    extra = jnp.logical_and(jnp.logical_not(is_hot), adjusted < leftover)
    counts = counts + extra.astype(jnp.int32)
    counts = jnp.where(is_hot, most, counts)
    ends = jnp.cumsum(counts, axis=1)
    starts = ends - counts
    place = jnp.arange(TOK_DEV, dtype=jnp.int32)
    owner_of = jnp.sum((place[None, :, None] >= ends[:, None, :]).astype(jnp.int32), axis=2)
    within = place[None, :] - jnp.take_along_axis(starts, owner_of, axis=1)
    own_count = jnp.take_along_axis(counts, owner_of, axis=1)
    reach = jnp.maximum(jnp.minimum(room, (3 * own_count + 3) // 4), 1)
    guess = jax.random.randint(keys[3], (N_DP, TOK_DEV), 0, reach, dtype=jnp.int32)
    slot = jnp.where(within < reach, within, guess)
    shuffle = jax.vmap(lambda k: jax.random.permutation(k, room))(jax.random.split(keys[4], N_DP * N_DP)).astype(jnp.int32).reshape(N_DP, N_DP, room)
    offset = jax.random.randint(keys[5], (N_DP, N_DP, room), 0, spread, dtype=jnp.int32)
    device = jnp.arange(N_DP, dtype=jnp.int32)[:, None]
    local_row = shuffle[device, owner_of, slot] * spread + offset[device, owner_of, slot]
    rows = owner_of * ROWS_DEV + local_row
    mixing = jax.vmap(lambda k: jax.random.permutation(k, TOK_DEV))(jax.random.split(keys[6], N_DP)).astype(jnp.int32)
    rows = jnp.take_along_axis(rows, mixing, axis=1)
    return rows.reshape(TOKENS).astype(jnp.int32)


def block_scale(key, shape, cuts, least, largest):
    gain, own = 1.0, jax.random.fold_in(key, 6)
    for dim, shards_of in cuts:
        draws = jnp.exp(jax.random.uniform(jax.random.fold_in(own, dim), (shards_of,), jnp.float32, least / len(cuts), largest / len(cuts)))
        gain = gain * jnp.repeat(draws, shape[dim] // shards_of).reshape([-1 if axis == dim else 1 for axis in range(len(shape))])
    return gain


def bell_draw(stream_key, extent, scale, most, cuts=(), kind=jnp.bfloat16):
    entries = jax.random.normal(stream_key, extent, jnp.float32) * scale
    if len(cuts) > 0:
        entries = block_scale(stream_key, extent, cuts, -0.22, 0.18) * entries
    return jnp.clip(entries, min=-most, max=most).astype(kind)


def setup_inputs(seed: int = 0) -> dict:
    key_list = jax.random.split(jax.random.key(seed), 6)
    table = bell_draw(key_list[0], (ROWS, D), 1.0, 6.0, ((0, 32), (1, 4)), jnp.float32)
    first_moment = bell_draw(key_list[1], (ROWS, D), 0.3, 1.8, ((0, 32), (1, 4)), jnp.float32)
    second_moment = jnp.clip(jnp.exp(math.log(1.0) - 4.6051702 * jax.random.uniform(key_list[2], (ROWS, D), jnp.float32) ** block_scale(key_list[2], (ROWS, D), ((0, 32), (1, 4)), -0.2, 0.2)), 0.01, 1.0)
    grads = draw_grads(jax.random.fold_in(key_list[5], 71), 0)
    ids = draw_ids(jax.random.fold_in(key_list[5], 71), 0)
    return {"table": table, "first_moment": first_moment, "second_moment": second_moment, "grads": grads, "ids": ids}


first_fix = 0.9999734386
second_fix = 0.0952078529

def reference(table, first_moment, second_moment, grads, ids):
    grad_rows = jax.ops.segment_sum(grads.astype(jnp.float32), ids, num_segments=ROWS)
    total = jnp.sum(grad_rows * grad_rows)
    limit = jnp.sqrt(jnp.float32(TOKENS * D))
    scale = limit / jnp.maximum(jnp.sqrt(total), limit)
    clipped = scale * grad_rows
    new_first = 0.9 * first_moment + 0.1 * clipped
    new_second = 0.999 * second_moment + 0.001 * clipped * clipped
    first_hat = new_first / first_fix
    second_hat = new_second / second_fix
    new_table = table - 0.01 * (first_hat / (jnp.sqrt(second_hat) + 1e-08) + 0.1 * table)
    return (new_table, new_first, new_second)
```

```python
import functools

import jax
import jax.numpy as jnp
from jax import lax
from jax.experimental import pallas as pl
from jax.experimental.pallas import tpu as pltpu
from jax.sharding import PartitionSpec as P

beta_first = 0.9
beta_second = 0.999
learn_rate = 0.01
decay_rate = 0.1
adam_eps = 1e-08
first_fix = 0.9999734386
second_fix = 0.0952078529

LANES = 128
ROOM = 64
TILE = 256
FAN = TILE // ROOM
MESH = pl.DeviceIdType.MESH
BIG = 1 << 30


def one_hot(index, base, rows):
    local = index - base
    local = jnp.where(jnp.logical_and(local >= 0, local < rows), local, -1)
    local = local.astype(jnp.float32).astype(jnp.bfloat16)
    shape = (rows, index.shape[1])
    here = lax.broadcasted_iota(jnp.int32, shape, 0).astype(jnp.float32).astype(jnp.bfloat16)
    return jnp.where(here == local, jnp.bfloat16(1), jnp.bfloat16(0))


def rank_tokens(ids_ref, spread_ref, joined_ref, dest_ref, rows_dev):
    blocks = ids_ref.shape[0]
    ids = ids_ref[...]
    columns = ids.T
    lane = lax.broadcasted_iota(jnp.int32, (LANES, LANES), 1)
    place = lax.broadcasted_iota(jnp.int32, (LANES, LANES), 0)
    for i in range(blocks):
        mine = jnp.broadcast_to(columns[:, i : i + 1], (LANES, LANES))
        local = mine & (rows_dev - 1)
        marks = jnp.where(lane == 0, local >> 6, jnp.where(lane == 1, local & 63, 1))
        marks = jnp.where(lane < 3, marks, 0)
        joined_ref[i * LANES : (i + 1) * LANES, LANES:] = marks.astype(jnp.float32).astype(jnp.bfloat16)
        seen = jnp.logical_and(mine == ids[i : i + 1, :], lane < place)
        for j in range(i):
            seen = jnp.logical_or(seen, mine == ids[j : j + 1, :])
        repeat = jnp.max(jnp.where(seen, 1.0, 0.0), axis=1, keepdims=True)
        spread_ref[i * LANES : (i + 1) * LANES, :] = jnp.where(repeat > 0.0, BIG, mine)

    queries = [jnp.broadcast_to(ids[j : j + 1, :], (8, LANES)) for j in range(blocks)]
    queries.append(lax.broadcasted_iota(jnp.int32, (8, LANES), 1) * rows_dev)

    def count(step, sums):
        for u in range(2):
            other = spread_ref[pl.ds(pl.multiple_of(step * 16, 16) + 8 * u, 8), :]
            sums = tuple(s + jnp.where(other < q, 1, 0) for s, q in zip(sums, queries))
        return sums

    zero = jnp.zeros((8, LANES), jnp.int32)
    sums = lax.fori_loop(0, blocks * LANES // 16, count, (zero,) * (blocks + 1))
    below = [jnp.sum(s.astype(jnp.float32), axis=0, keepdims=True).astype(jnp.int32) for s in sums]
    start = jnp.broadcast_to(below[-1], (8, LANES))
    for j in range(blocks):
        owner = ids[j : j + 1, :] // rows_dev
        first = jnp.take_along_axis(start, jnp.broadcast_to(owner, (8, LANES)), axis=1)[0:1, :]
        dest_ref[:, j * LANES : (j + 1) * LANES] = owner * ROOM + below[j] - first


def exchange_kernel(
    n, others, ids_ref, grads_ref, rows_ref, total_ref,
    spread_ref, joined_ref, dest_ref, sums_ref, marks_ref, got_ref, got_marks_ref, split_ref,
    part_ref, parts_ref, plane_ref, planes_ref,
    load_sem, sums_send, sums_recv, marks_send, marks_recv, part_send, part_recv, plane_send, plane_recv,
):
    me = lax.axis_index("dp")
    col = lax.axis_index("mp")
    groups = n // FAN
    rows_dev = rows_ref.shape[0]
    my_group = me // FAN

    barrier = pltpu.get_barrier_semaphore()

    def greet(step, carry):
        pl.semaphore_signal(barrier, inc=1, device_id={"dp": lax.rem(me + step, n)}, device_id_type=MESH)
        return carry

    lax.fori_loop(1, n, greet, 0)
    for step in range(1, others):
        pl.semaphore_signal(barrier, inc=1, device_id={"mp": lax.rem(col + step, others)}, device_id_type=MESH)

    load = pltpu.make_async_copy(grads_ref, joined_ref.at[:, 0:LANES], load_sem)
    load.start()
    rank_tokens(ids_ref, spread_ref, joined_ref, dest_ref, rows_dev)
    load.wait()
    pl.semaphore_wait(barrier, n - 1 + others - 1)

    def sums_copy(peer, source):
        return pltpu.make_async_remote_copy(
            src_ref=sums_ref.at[peer], dst_ref=got_ref.at[source],
            send_sem=sums_send.at[peer], recv_sem=sums_recv.at[source],
            device_id={"dp": peer}, device_id_type=MESH,
        )

    def marks_copy(peer, source):
        return pltpu.make_async_remote_copy(
            src_ref=marks_ref.at[peer // 2], dst_ref=got_marks_ref.at[source],
            send_sem=marks_send.at[peer], recv_sem=marks_recv.at[source],
            device_id={"dp": peer}, device_id_type=MESH,
        )

    def pack(k, carry):
        tile = lax.rem(my_group + k, groups)
        hot = one_hot(dest_ref[...], tile * TILE, TILE)
        out = jnp.dot(hot, joined_ref[...], preferred_element_type=jnp.float32)
        for a in range(FAN):
            sums_ref[FAN * tile + a] = out[a * ROOM : (a + 1) * ROOM, :LANES]
        for h in range(2):
            turned = out[h * LANES : (h + 1) * LANES, LANES:].T
            times = turned[2:3, :]
            row = (turned[0:1, :] * 64.0 + turned[1:2, :]) / jnp.maximum(times, 1.0)
            marks_ref[2 * tile + h] = jnp.where(times > 0.0, jnp.floor(row + 0.5), -1.0)
        for a in range(FAN):
            peer = FAN * tile + a

            @pl.when(peer != me)
            def _():
                marks_copy(peer, me).start()
                sums_copy(peer, me).start()

        return carry

    lax.fori_loop(0, groups, pack, 0)
    got_ref[me] = sums_ref[me]
    got_marks_ref[me] = marks_ref[me // 2]

    half = lax.rem(me, 2)
    lane = lax.broadcasted_iota(jnp.int32, (1, LANES), 1)

    def take(k, first, last):
        group = lax.rem(my_group - k + groups, groups)
        for a in range(FAN):
            source = FAN * group + a

            @pl.when(source != me)
            def _():
                marks_copy(me, source).wait_recv()
                sums_copy(me, source).wait_recv()

        pieces = []
        for h in range(2):
            left = got_marks_ref[FAN * group + 2 * h]
            right = got_marks_ref[FAN * group + 2 * h + 1]
            low = jnp.where(lane < ROOM, left, pltpu.roll(right, ROOM, 1))
            high = jnp.where(lane < ROOM, pltpu.roll(left, ROOM, 1), right)
            pieces.append(jnp.where(half == 0, low, high))
        marks = jnp.concatenate(pieces, axis=1).astype(jnp.int32)
        for a in range(FAN):
            value = got_ref[FAN * group + a]
            big = value.astype(jnp.bfloat16)
            split_ref[a * ROOM : (a + 1) * ROOM, :LANES] = big
            split_ref[a * ROOM : (a + 1) * ROOM, LANES:] = (value - big.astype(jnp.float32)).astype(jnp.bfloat16)

        def spread(step, squares):
            for u in range(2):
                base = pl.multiple_of((step * 2 + u) * TILE, TILE)
                hot = one_hot(marks, base, TILE)
                out = jnp.dot(hot, split_ref[...], preferred_element_type=jnp.float32)
                rows = out[:, :LANES] + out[:, LANES:]
                if not first:
                    rows = rows + rows_ref[pl.ds(base, TILE), :]
                rows_ref[pl.ds(base, TILE), :] = rows
                if last:
                    squares = squares + jnp.sum((rows * rows).reshape(TILE // 8, 8, LANES), axis=0)
            return squares

        return lax.fori_loop(0, rows_dev // TILE // 2, spread, jnp.zeros((8, LANES), jnp.float32))

    take(0, True, False)
    lax.fori_loop(1, groups - 1, lambda k, c: (take(k, False, False), c)[1], 0)
    squares = take(groups - 1, False, True)

    part_ref[...] = jnp.sum(squares, axis=0, keepdims=True)
    parts_ref[me] = part_ref[...]

    def part_copy(peer, source):
        return pltpu.make_async_remote_copy(
            src_ref=part_ref, dst_ref=parts_ref.at[source],
            send_sem=part_send.at[peer], recv_sem=part_recv.at[source],
            device_id={"dp": peer}, device_id_type=MESH,
        )

    def plane_copy(peer, source):
        return pltpu.make_async_remote_copy(
            src_ref=plane_ref, dst_ref=planes_ref.at[source],
            send_sem=plane_send.at[peer], recv_sem=plane_recv.at[source],
            device_id={"mp": peer}, device_id_type=MESH,
        )

    def each_peer(act):
        def one(step, carry):
            act(lax.rem(me + step, n))
            return carry

        lax.fori_loop(1, n, one, 0)

    each_peer(lambda peer: part_copy(peer, me).start())
    each_peer(lambda peer: part_copy(me, peer).wait_recv())
    plane_ref[...] = jnp.sum(parts_ref[...], axis=0)
    planes_ref[col] = plane_ref[...]
    for step in range(1, others):
        plane_copy(lax.rem(col + step, others), col).start()
    for step in range(1, others):
        plane_copy(col, lax.rem(col + step, others)).wait_recv()
    total_ref[...] = jnp.sum(planes_ref[...], axis=0)

    def drain(peer):
        marks_copy(peer, me).wait_send()
        sums_copy(peer, me).wait_send()
        part_copy(peer, me).wait_send()

    each_peer(drain)
    for step in range(1, others):
        plane_copy(lax.rem(col + step, others), col).wait_send()


def update_kernel(limit, total_ref, rows_ref, table_ref, first_ref, second_ref, new_table_ref, new_first_ref, new_second_ref):
    total = jnp.sum(total_ref[...], axis=1, keepdims=True)
    scale = limit / jnp.maximum(jnp.sqrt(total), limit)
    clipped = scale * rows_ref[...]
    first = beta_first * first_ref[...] + (1.0 - beta_first) * clipped
    second = beta_second * second_ref[...] + (1.0 - beta_second) * clipped * clipped
    new_first_ref[...] = first
    new_second_ref[...] = second
    root = second_fix**0.5
    step = (learn_rate * root / first_fix) * first / (jnp.sqrt(second) + adam_eps * root)
    new_table_ref[...] = (1.0 - learn_rate * decay_rate) * table_ref[...] - step


def body(table, first_moment, second_moment, grads, ids):
    n = lax.axis_size("dp")
    others = lax.axis_size("mp")
    rows_dev, width = table.shape
    tok_dev = grads.shape[0]
    slots = n * ROOM
    groups = n // FAN
    dma = pltpu.SemaphoreType.DMA
    rows, total = pl.pallas_call(
        functools.partial(exchange_kernel, n, others),
        out_shape=(
            jax.ShapeDtypeStruct((rows_dev, width), jnp.float32),
            jax.ShapeDtypeStruct((1, LANES), jnp.float32),
        ),
        in_specs=[pl.BlockSpec(memory_space=pltpu.VMEM), pl.BlockSpec(memory_space=pl.ANY)],
        out_specs=(pl.BlockSpec(memory_space=pltpu.VMEM), pl.BlockSpec(memory_space=pltpu.VMEM)),
        scratch_shapes=[
            pltpu.VMEM((tok_dev, LANES), jnp.int32),
            pltpu.VMEM((tok_dev, 2 * LANES), jnp.bfloat16),
            pltpu.VMEM((1, tok_dev), jnp.int32),
            pltpu.VMEM((n, ROOM, width), jnp.float32),
            pltpu.VMEM((n // 2, 1, LANES), jnp.float32),
            pltpu.VMEM((n, ROOM, width), jnp.float32),
            pltpu.VMEM((n, 1, LANES), jnp.float32),
            pltpu.VMEM((TILE, 2 * LANES), jnp.bfloat16),
            pltpu.VMEM((1, LANES), jnp.float32),
            pltpu.VMEM((n, 1, LANES), jnp.float32),
            pltpu.VMEM((1, LANES), jnp.float32),
            pltpu.VMEM((others, 1, LANES), jnp.float32),
            dma,
            dma((n,)),
            dma((n,)),
            dma((n,)),
            dma((n,)),
            dma((n,)),
            dma((n,)),
            dma((others,)),
            dma((others,)),
        ],
        compiler_params=pltpu.CompilerParams(
            collective_id=0, has_side_effects=True, vmem_limit_bytes=24 * 1024 * 1024
        ),
    )(ids.reshape(tok_dev // LANES, LANES), grads)

    limit = float(tok_dev * n * width * others) ** 0.5
    chunk = 512
    block = pl.BlockSpec((chunk, width), lambda i: (i, 0))
    shape = jax.ShapeDtypeStruct((rows_dev, width), jnp.float32)
    return pl.pallas_call(
        functools.partial(update_kernel, limit),
        grid=(rows_dev // chunk,),
        out_shape=(shape, shape, shape),
        in_specs=[pl.BlockSpec((1, LANES), lambda i: (0, 0)), block, block, block, block],
        out_specs=(block, block, block),
        compiler_params=pltpu.CompilerParams(vmem_limit_bytes=16 * 1024 * 1024),
    )(total, rows, table, first_moment, second_moment)


def solution(mesh):
    placed = (P("dp", "mp"), P("dp", "mp"), P("dp", "mp"), P("dp", "mp"), P("dp"))
    return jax.shard_map(
        body,
        mesh=mesh,
        in_specs=placed,
        out_specs=(P("dp", "mp"), P("dp", "mp"), P("dp", "mp")),
        check_vma=False,
    )
```

```python
import functools

import jax
import jax.numpy as jnp
from jax import lax
from jax.experimental import pallas as pl
from jax.experimental.pallas import tpu as pltpu
from jax.sharding import PartitionSpec as P

beta_first = 0.9
beta_second = 0.999
learn_rate = 0.01
decay_rate = 0.1
adam_eps = 1e-08
first_fix = 0.9999734386
second_fix = 0.0952078529

LANES = 128
ROOM = 64
TILE = 256
FAN = TILE // ROOM
MESH = pl.DeviceIdType.MESH
BIG = 1 << 30


def one_hot(index, base, rows):
    local = index - base
    local = jnp.where(jnp.logical_and(local >= 0, local < rows), local, -1)
    local = local.astype(jnp.float32).astype(jnp.bfloat16)
    shape = (rows, index.shape[1])
    here = lax.broadcasted_iota(jnp.int32, shape, 0).astype(jnp.float32).astype(jnp.bfloat16)
    return jnp.where(here == local, jnp.bfloat16(1), jnp.bfloat16(0))


def rank_tokens(ids_ref, spread_ref, joined_ref, dest_ref, rows_dev):
    blocks = ids_ref.shape[0]
    ids = ids_ref[...]
    columns = ids.T
    lane = lax.broadcasted_iota(jnp.int32, (LANES, LANES), 1)
    place = lax.broadcasted_iota(jnp.int32, (LANES, LANES), 0)
    shift = jnp.where(lane == 0, 6, 0)
    keep = jnp.where(lane == 0, rows_dev // 64 - 1, jnp.where(lane == 1, 63, 0))
    one = jnp.where(lane == 2, 1, 0)
    later = jnp.where(lane < place, 0.0, 1.0)
    for i in range(blocks):
        mine = jnp.broadcast_to(columns[:, i : i + 1], (LANES, LANES))
        marks = (lax.shift_right_logical(mine, shift) & keep) | one
        joined_ref[i * LANES : (i + 1) * LANES, LANES:] = marks.astype(jnp.float32).astype(jnp.bfloat16)
        alone = jnp.where(mine == ids[i : i + 1, :], later, 1.0)
        for j in range(i):
            alone = jnp.where(mine == ids[j : j + 1, :], 0.0, alone)
        least = jnp.min(alone, axis=1, keepdims=True)
        spread_ref[i * LANES : (i + 1) * LANES, :] = jnp.where(least > 0.0, mine, BIG)

    queries = [jnp.broadcast_to(ids[j : j + 1, :], (8, LANES)) for j in range(blocks)]
    queries.append(lax.broadcasted_iota(jnp.int32, (8, LANES), 1) * rows_dev)
    sums = []
    for part in (queries[:9], queries[9:]):

        def count(step, found, part=part):
            for u in range(8):
                other = spread_ref[pl.ds(pl.multiple_of(step * 64, 64) + 8 * u, 8), :]
                found = tuple(f + lax.shift_right_logical(other - q, 31) for f, q in zip(found, part))
            return found

        zero = jnp.zeros((8, LANES), jnp.int32)
        sums.extend(lax.fori_loop(0, blocks * LANES // 64, count, (zero,) * len(part)))
    below = [jnp.sum(s.astype(jnp.float32), axis=0, keepdims=True).astype(jnp.int32) for s in sums]
    start = jnp.broadcast_to(below[-1], (8, LANES))
    for j in range(blocks):
        owner = ids[j : j + 1, :] // rows_dev
        first = jnp.take_along_axis(start, jnp.broadcast_to(owner, (8, LANES)), axis=1)[0:1, :]
        dest_ref[:, j * LANES : (j + 1) * LANES] = owner * ROOM + below[j] - first


def stages(groups):
    return [groups // 2, groups * 3 // 4, groups - 1, groups]


def exchange_kernel(
    n, others, rows_dev, ids_hbm, grads_ref, all_ref, where_ref, total_ref,
    ids_ref, spread_ref, joined_ref, dest_ref, sums_ref, marks_ref, got_ref, got_marks_ref, split_ref, names_ref, tags_ref,
    part_ref, parts_ref, plane_ref, planes_ref,
    load_sem, ids_sem, sums_send, sums_recv, marks_send, marks_recv, part_send, part_recv, plane_send, plane_recv,
):
    me = lax.axis_index("dp")
    col = lax.axis_index("mp")
    groups = n // FAN
    my_group = me // FAN

    ids_load = pltpu.make_async_copy(ids_hbm, ids_ref, ids_sem)
    ids_load.start()
    load = pltpu.make_async_copy(grads_ref, joined_ref.at[:, 0:LANES], load_sem)
    load.start()
    barrier = pltpu.get_barrier_semaphore()

    def greet(step, carry):
        pl.semaphore_signal(barrier, inc=1, device_id={"dp": lax.rem(me + step, n)}, device_id_type=MESH)
        return carry

    lax.fori_loop(1, n, greet, 0)
    for step in range(1, others):
        pl.semaphore_signal(barrier, inc=1, device_id={"mp": lax.rem(col + step, others)}, device_id_type=MESH)

    ids_load.wait()
    rank_tokens(ids_ref, spread_ref, joined_ref, dest_ref, rows_dev)
    load.wait()
    pl.semaphore_wait(barrier, n - 1 + others - 1)

    def sums_copy(peer, source, place):
        return pltpu.make_async_remote_copy(
            src_ref=sums_ref.at[peer], dst_ref=got_ref.at[place],
            send_sem=sums_send.at[peer], recv_sem=sums_recv.at[place],
            device_id={"dp": peer}, device_id_type=MESH,
        )

    def marks_copy(peer, source, place):
        return pltpu.make_async_remote_copy(
            src_ref=marks_ref.at[peer // 2], dst_ref=got_marks_ref.at[place],
            send_sem=marks_send.at[peer], recv_sem=marks_recv.at[place],
            device_id={"dp": peer}, device_id_type=MESH,
        )

    seat = lax.rem(me, FAN)

    def pack(k, carry):
        tile = lax.rem(my_group + k, groups)
        hot = one_hot(dest_ref[...], tile * TILE, TILE)
        out = jnp.dot(hot, joined_ref[...], preferred_element_type=jnp.float32)
        for a in range(FAN):
            sums_ref[FAN * tile + a] = out[a * ROOM : (a + 1) * ROOM, :LANES]
        for h in range(2):
            turned = out[h * LANES : (h + 1) * LANES, LANES:].T
            times = turned[2:3, :]
            row = (turned[0:1, :] * 64.0 + turned[1:2, :]) / jnp.maximum(times, 1.0)
            marks_ref[2 * tile + h] = jnp.where(times > 0.0, jnp.floor(row + 0.5), -1.0)
        for a in range(FAN):
            peer = FAN * tile + a

            @pl.when(peer != me)
            def _():
                marks_copy(peer, me, FAN * k + seat).start()
                sums_copy(peer, me, FAN * k + seat).start()

        return carry

    lax.fori_loop(0, groups, pack, 0)
    got_ref[seat] = sums_ref[me]
    got_marks_ref[seat] = marks_ref[me // 2]

    half = lax.rem(me, 2)
    low_lane = lax.broadcasted_iota(jnp.int32, (1, LANES), 1) < ROOM

    def arrive(k):
        for a in range(FAN):
            if k == 0:

                @pl.when(a != seat)
                def _():
                    marks_copy(me, me, a).wait_recv()
                    sums_copy(me, me, a).wait_recv()
            else:
                marks_copy(me, me, FAN * k + a).wait_recv()
                sums_copy(me, me, FAN * k + a).wait_recv()
        for h in range(2):
            left = got_marks_ref[FAN * k + 2 * h]
            right = got_marks_ref[FAN * k + 2 * h + 1]
            low = jnp.where(low_lane, left, pltpu.roll(right, ROOM, 1))
            high = jnp.where(low_lane, pltpu.roll(left, ROOM, 1), right)
            row = jnp.where(half == 0, low, high)
            names_ref[:, k * TILE + h * LANES : k * TILE + (h + 1) * LANES] = row
            tags_ref[k * TILE + h * LANES : k * TILE + (h + 1) * LANES, :] = jnp.broadcast_to(row, (LANES, LANES)).T
            where_ref[2 * k + h : 2 * k + h + 1, :] = jnp.where(row < 0.0, float(rows_dev), row).astype(jnp.int32)
        for a in range(FAN):
            value = got_ref[FAN * k + a]
            big = value.astype(jnp.bfloat16)
            at = pl.ds(k * TILE + a * ROOM, ROOM)
            split_ref[at, :LANES] = big
            split_ref[at, LANES:] = (value - big.astype(jnp.float32)).astype(jnp.bfloat16)

    def match(rows, first, last):
        tags = tags_ref[rows, :]
        hot = [
            jnp.where(tags == names_ref[:, c * LANES : (c + 1) * LANES], 1.0, 0.0).astype(jnp.bfloat16)
            for c in range(first * 2, last * 2)
        ]
        hot = jnp.concatenate(hot, axis=1)
        out = jnp.dot(hot, split_ref[first * TILE : last * TILE, :], preferred_element_type=jnp.float32)
        return out[:, :LANES] + out[:, LANES:]

    def tile_rows(i):
        return pl.ds(pl.multiple_of(i * TILE, TILE), TILE)

    def fresh(i, last):
        all_ref[tile_rows(i), :] = match(tile_rows(i), 0, last)

    def more(i, first, last):
        all_ref[tile_rows(i), :] += match(tile_rows(i), first, last)

    def over(low, high, act):
        lax.fori_loop(low, high, lambda i, c: (act(i), c)[1], 0)

    done = 0
    for last in stages(groups):
        for k in range(done, last):
            arrive(k)
        if last < groups - 1:
            if done > 0:
                over(0, done, lambda i: more(i, done, last))
            over(done, last, lambda i: fresh(i, last))
        else:
            for i in range(done):
                more(i, done, last)
            for i in range(done, last):
                fresh(i, last)
        done = last

    squares = jnp.zeros((8, LANES), jnp.float32)
    for k in range(groups):
        for a in range(FAN):
            at = k * TILE + a * ROOM
            both = got_ref[FAN * k + a] * all_ref[at : at + ROOM, :]
            squares = squares + jnp.sum(both.reshape(ROOM // 8, 8, LANES), axis=0)

    part_ref[...] = jnp.sum(squares, axis=0, keepdims=True)
    parts_ref[me] = part_ref[...]

    def part_copy(peer, source):
        return pltpu.make_async_remote_copy(
            src_ref=part_ref, dst_ref=parts_ref.at[source],
            send_sem=part_send.at[peer], recv_sem=part_recv.at[source],
            device_id={"dp": peer}, device_id_type=MESH,
        )

    def plane_copy(peer, source):
        return pltpu.make_async_remote_copy(
            src_ref=plane_ref, dst_ref=planes_ref.at[source],
            send_sem=plane_send.at[peer], recv_sem=plane_recv.at[source],
            device_id={"mp": peer}, device_id_type=MESH,
        )

    def each_peer(act):
        def one(step, carry):
            act(lax.rem(me + step, n))
            return carry

        lax.fori_loop(1, n, one, 0)

    each_peer(lambda peer: part_copy(peer, me).start())
    each_peer(lambda peer: part_copy(me, peer).wait_recv())
    plane_ref[...] = jnp.sum(parts_ref[...], axis=0)
    planes_ref[col] = plane_ref[...]
    for step in range(1, others):
        plane_copy(lax.rem(col + step, others), col).start()
    for step in range(1, others):
        plane_copy(col, lax.rem(col + step, others)).wait_recv()
    total_ref[...] = jnp.sum(planes_ref[...], axis=0)

    def drain(peer):
        marks_copy(peer, me, 0).wait_send()
        sums_copy(peer, me, 0).wait_send()
        part_copy(peer, me).wait_send()

    each_peer(drain)
    for step in range(1, others):
        plane_copy(lax.rem(col + step, others), col).wait_send()


def update_kernel(
    limit, total_ref, where_hbm, all_ref, table_ref, first_ref, second_ref, new_table_hbm, new_first_hbm, new_second_hbm,
    where_ref, rows_ref, new_table_ref, new_first_ref, new_second_ref, where_sem, out_sem,
):
    load = pltpu.make_async_copy(where_hbm, where_ref, where_sem)
    load.start()
    rows_dev = table_ref.shape[0]
    chunk = 512

    def clear(i, carry):
        rows_ref[pl.ds(pl.multiple_of(i * chunk, chunk), chunk), :] = jnp.zeros((chunk, LANES), jnp.float32)
        return carry

    lax.fori_loop(0, rows_dev // chunk, clear, 0)
    total = jnp.sum(total_ref[...], axis=1, keepdims=True)
    scale = limit / jnp.maximum(jnp.sqrt(total), limit)
    load.wait()

    def place(i, carry):
        base = pl.multiple_of(i * LANES, LANES)
        for u in range(LANES):
            rows_ref[pl.ds(where_ref[i, u], 1), :] = all_ref[pl.ds(base + u, 1), :]
        return carry

    lax.fori_loop(0, all_ref.shape[0] // LANES, place, 0)

    def outs(i):
        at = pl.ds(pl.multiple_of(i * chunk, chunk), chunk)
        return [
            pltpu.make_async_copy(ref.at[at, :], hbm.at[at, :], out_sem.at[w, i])
            for w, (ref, hbm) in enumerate(
                [(new_table_ref, new_table_hbm), (new_first_ref, new_first_hbm), (new_second_ref, new_second_hbm)]
            )
        ]

    root = second_fix**0.5

    def update(i, carry):
        at = pl.ds(pl.multiple_of(i * chunk, chunk), chunk)
        clipped = scale * rows_ref[at, :]
        first = beta_first * first_ref[at, :] + (1.0 - beta_first) * clipped
        second = beta_second * second_ref[at, :] + (1.0 - beta_second) * clipped * clipped
        new_first_ref[at, :] = first
        new_second_ref[at, :] = second
        step = (learn_rate * root / first_fix) * first / (second * lax.rsqrt(second) + adam_eps * root)
        new_table_ref[at, :] = (1.0 - learn_rate * decay_rate) * table_ref[at, :] - step
        for copy in outs(i):
            copy.start()
        return carry

    lax.fori_loop(0, rows_dev // chunk, update, 0)

    def finish(i, carry):
        for copy in outs(i):
            copy.wait()
        return carry

    lax.fori_loop(0, rows_dev // chunk, finish, 0)


def body(table, first_moment, second_moment, grads, ids):
    n = lax.axis_size("dp")
    others = lax.axis_size("mp")
    rows_dev, width = table.shape
    tok_dev = grads.shape[0]
    slots = n * ROOM
    dma = pltpu.SemaphoreType.DMA
    vmem = pl.BlockSpec(memory_space=pltpu.VMEM)
    hbm = pl.BlockSpec(memory_space=pltpu.HBM)
    anywhere = pl.BlockSpec(memory_space=pl.ANY)
    sums, where, total = pl.pallas_call(
        functools.partial(exchange_kernel, n, others, rows_dev),
        out_shape=(
            jax.ShapeDtypeStruct((slots, width), jnp.float32),
            jax.ShapeDtypeStruct((slots // LANES, LANES), jnp.int32),
            jax.ShapeDtypeStruct((1, LANES), jnp.float32),
        ),
        in_specs=[hbm, hbm],
        out_specs=(vmem, vmem, vmem),
        scratch_shapes=[
            pltpu.VMEM((tok_dev // LANES, LANES), jnp.int32),
            pltpu.VMEM((tok_dev, LANES), jnp.int32),
            pltpu.VMEM((tok_dev, 2 * LANES), jnp.bfloat16),
            pltpu.VMEM((1, tok_dev), jnp.int32),
            pltpu.VMEM((n, ROOM, width), jnp.float32),
            pltpu.VMEM((n // 2, 1, LANES), jnp.float32),
            pltpu.VMEM((n, ROOM, width), jnp.float32),
            pltpu.VMEM((n, 1, LANES), jnp.float32),
            pltpu.VMEM((slots, 2 * LANES), jnp.bfloat16),
            pltpu.VMEM((1, slots), jnp.float32),
            pltpu.VMEM((slots, LANES), jnp.float32),
            pltpu.VMEM((1, LANES), jnp.float32),
            pltpu.VMEM((n, 1, LANES), jnp.float32),
            pltpu.VMEM((1, LANES), jnp.float32),
            pltpu.VMEM((others, 1, LANES), jnp.float32),
            dma,
            dma,
            dma((n,)),
            dma((n,)),
            dma((n,)),
            dma((n,)),
            dma((n,)),
            dma((n,)),
            dma((others,)),
            dma((others,)),
        ],
        compiler_params=pltpu.CompilerParams(
            collective_id=0, has_side_effects=True, vmem_limit_bytes=20 * 1024 * 1024
        ),
        cost_estimate=pl.CostEstimate(flops=10**11, bytes_accessed=10**8, transcendentals=0),
    )(ids.reshape(tok_dev // LANES, LANES), grads)

    limit = float(tok_dev * n * width * others) ** 0.5
    shape = jax.ShapeDtypeStruct((rows_dev, width), jnp.float32)
    chunks = rows_dev // 512
    return pl.pallas_call(
        functools.partial(update_kernel, limit),
        out_shape=(shape, shape, shape),
        in_specs=[vmem, anywhere, vmem, vmem, vmem, vmem],
        out_specs=(hbm, hbm, hbm),
        scratch_shapes=[
            pltpu.SMEM((slots // LANES, LANES), jnp.int32),
            pltpu.VMEM((rows_dev + 8, width), jnp.float32),
            pltpu.VMEM((rows_dev, width), jnp.float32),
            pltpu.VMEM((rows_dev, width), jnp.float32),
            pltpu.VMEM((rows_dev, width), jnp.float32),
            dma,
            dma((3, chunks)),
        ],
        compiler_params=pltpu.CompilerParams(vmem_limit_bytes=40 * 1024 * 1024),
    )(total, where, sums, table, first_moment, second_moment)


def solution(mesh):
    placed = (P("dp", "mp"), P("dp", "mp"), P("dp", "mp"), P("dp", "mp"), P("dp"))
    return jax.shard_map(
        body,
        mesh=mesh,
        in_specs=placed,
        out_specs=(P("dp", "mp"), P("dp", "mp"), P("dp", "mp")),
        check_vma=False,
    )
```

```python
import functools

import jax
import jax.numpy as jnp
from jax import lax
from jax.experimental import pallas as pl
from jax.experimental.pallas import tpu as pltpu
from jax.sharding import PartitionSpec as P

beta_first = 0.9
beta_second = 0.999
learn_rate = 0.01
decay_rate = 0.1
adam_eps = 1e-08
first_fix = 0.9999734386
second_fix = 0.0952078529

LANES = 128
ROOM = 64
TILE = 256
FAN = TILE // ROOM
MESH = pl.DeviceIdType.MESH
BIG = 1 << 30
CODES = 32767.0


STEPS = [
    [(0, 0, 0), (0, 0, 1), (2, 2, 0), (2, 2, 1)],
    [(2, 1, 0), (1, 2, 0), (2, 3, 0), (3, 2, 0)],
    [(2, 1, 1), (1, 2, 1), (2, 3, 1), (3, 2, 1)],
    [(2, 0, 0), (0, 2, 0), (2, 0, 1), (0, 2, 1)],
    [(1, 1, 0), (3, 3, 0), (1, 3, 0), (3, 1, 0)],
    [(1, 1, 1), (3, 3, 1), (1, 3, 1), (3, 1, 1)],
    [(1, 0, 0), (3, 0, 0), (0, 1, 0), (0, 3, 0)],
    [(1, 0, 1), (3, 0, 1), (0, 1, 1), (0, 3, 1)],
]
SIDE = 4


def peer_of(me, offset):
    core = lax.rem(me, 2)
    z = lax.rem(me // 2, SIDE)
    y = me // (2 * SIDE)
    core = 1 - core if offset[2] else core
    return (lax.rem(y + offset[0], SIDE) * SIDE + lax.rem(z + offset[1], SIDE)) * 2 + core


def rank_tokens(ids_ref, spread_ref, joined_ref, owner_ref, slot_ref, rows_dev):
    blocks = ids_ref.shape[0]
    ids = ids_ref[...]
    columns = ids.T
    lane = lax.broadcasted_iota(jnp.int32, (LANES, LANES), 1)
    place = lax.broadcasted_iota(jnp.int32, (LANES, LANES), 0)
    shift = jnp.where(lane == 0, 6, 0)
    keep = jnp.where(lane == 0, rows_dev // 64 - 1, jnp.where(lane == 1, 63, 0))
    one = jnp.where(lane == 2, 1, 0)
    later = jnp.where(lane < place, 0.0, 1.0)
    for i in range(blocks):
        mine = jnp.broadcast_to(columns[:, i : i + 1], (LANES, LANES))
        marks = (lax.shift_right_logical(mine, shift) & keep) | one
        joined_ref[i * LANES : (i + 1) * LANES, LANES:] = marks.astype(jnp.float32).astype(jnp.bfloat16)
        alone = jnp.where(mine == ids[i : i + 1, :], later, 1.0)
        for j in range(i):
            alone = jnp.where(mine == ids[j : j + 1, :], 0.0, alone)
        least = jnp.min(alone, axis=1, keepdims=True)
        spread_ref[i * LANES : (i + 1) * LANES, :] = jnp.where(least > 0.0, mine, BIG)

    queries = [jnp.broadcast_to(ids[j : j + 1, :], (8, LANES)) for j in range(blocks)]
    queries.append(lax.broadcasted_iota(jnp.int32, (8, LANES), 1) * rows_dev)
    sums = []
    for part in (queries[:9], queries[9:]):

        def count(step, found, part=part):
            for u in range(8):
                other = spread_ref[pl.ds(pl.multiple_of(step * 64, 64) + 8 * u, 8), :]
                found = tuple(f + lax.shift_right_logical(other - q, 31) for f, q in zip(found, part))
            return found

        zero = jnp.zeros((8, LANES), jnp.int32)
        sums.extend(lax.fori_loop(0, blocks * LANES // 64, count, (zero,) * len(part)))
    below = [jnp.sum(s.astype(jnp.float32), axis=0, keepdims=True).astype(jnp.int32) for s in sums]
    start = jnp.broadcast_to(below[-1], (8, LANES))
    for j in range(blocks):
        owner = ids[j : j + 1, :] // rows_dev
        first = jnp.take_along_axis(start, jnp.broadcast_to(owner, (8, LANES)), axis=1)[0:1, :]
        owner_ref[:, j * LANES : (j + 1) * LANES] = owner
        slot_ref[:, j * LANES : (j + 1) * LANES] = below[j] - first


def stages(groups):
    return [groups // 2, groups * 3 // 4, groups - 1, groups]


def exchange_kernel(
    n, others, rows_dev, ids_hbm, grads_ref, all_ref, where_ref, total_ref,
    ids_ref, spread_ref, joined_ref, owner_ref, slot_ref, sums_ref, marks_ref, got_ref, got_marks_ref, split_ref,
    names_ref, gains_ref, tags_ref, factors_ref,
    part_ref, parts_ref, plane_ref, planes_ref,
    load_sem, ids_sem, sums_send, sums_recv, marks_send, marks_recv, part_send, part_recv, plane_send, plane_recv,
):
    me = lax.axis_index("dp")
    col = lax.axis_index("mp")
    groups = n // FAN

    ids_load = pltpu.make_async_copy(ids_hbm, ids_ref, ids_sem)
    ids_load.start()
    load = pltpu.make_async_copy(grads_ref, joined_ref.at[:, 0:LANES], load_sem)
    load.start()
    barrier = pltpu.get_barrier_semaphore()

    def greet(step, carry):
        pl.semaphore_signal(barrier, inc=1, device_id={"dp": lax.rem(me + step, n)}, device_id_type=MESH)
        return carry

    lax.fori_loop(1, n, greet, 0)
    for step in range(1, others):
        pl.semaphore_signal(barrier, inc=1, device_id={"mp": lax.rem(col + step, others)}, device_id_type=MESH)

    ids_load.wait()
    rank_tokens(ids_ref, spread_ref, joined_ref, owner_ref, slot_ref, rows_dev)
    load.wait()

    def sums_copy(peer, place):
        return pltpu.make_async_remote_copy(
            src_ref=sums_ref.at[place], dst_ref=got_ref.at[place],
            send_sem=sums_send.at[place], recv_sem=sums_recv.at[place],
            device_id={"dp": peer}, device_id_type=MESH,
        )

    def marks_copy(peer, place):
        return pltpu.make_async_remote_copy(
            src_ref=marks_ref.at[place // 2], dst_ref=got_marks_ref.at[place],
            send_sem=marks_send.at[place], recv_sem=marks_recv.at[place],
            device_id={"dp": peer}, device_id_type=MESH,
        )

    tokens = owner_ref.shape[1]
    here = lax.broadcasted_iota(jnp.int32, (TILE, tokens), 0).astype(jnp.float32).astype(jnp.bfloat16)
    lane = lax.broadcasted_iota(jnp.int32, (LANES, LANES), 1)

    for k in range(groups):
        peers = [peer_of(me, offset) for offset in STEPS[k]]
        owner = owner_ref[...]
        slot = slot_ref[...]
        row = jnp.full_like(slot, -1)
        for a in range(FAN):
            row = jnp.where(owner == peers[a], slot + a * ROOM, row)
        row = row.astype(jnp.float32).astype(jnp.bfloat16)
        hot = jnp.where(here == row, jnp.bfloat16(1), jnp.bfloat16(0))
        out = jnp.dot(hot, joined_ref[...], preferred_element_type=jnp.float32)
        for h in range(2):
            value = out[h * LANES : (h + 1) * LANES, :LANES]
            most = jnp.max(jnp.abs(value), axis=1, keepdims=True)
            unit = jnp.maximum(most * ((1.0 + 2.0**-7) / CODES), 1e-30).astype(jnp.bfloat16).astype(jnp.float32)
            code = jnp.clip(jnp.round(value * (1.0 / unit)), -CODES, CODES).astype(jnp.int32).astype(jnp.int16)
            for a in range(2):
                sums_ref[FAN * k + 2 * h + a] = code[a * ROOM : (a + 1) * ROOM, :]
            turned = jnp.where(lane == 3, unit, out[h * LANES : (h + 1) * LANES, LANES:]).T
            times = turned[2:3, :]
            name = (turned[0:1, :] * 64.0 + turned[1:2, :]) / jnp.maximum(times, 1.0)
            marks_ref[2 * k + h, 0:1, :] = jnp.where(times > 0.0, jnp.floor(name + 0.5), -1.0)
            marks_ref[2 * k + h, 1:2, :] = turned[3:4, :]
        if k == 0:
            pl.semaphore_wait(barrier, n - 1 + others - 1)
        for a in range(FAN):
            if k + a > 0:
                marks_copy(peers[a], FAN * k + a).start()
                sums_copy(peers[a], FAN * k + a).start()

    got_ref[0] = sums_ref[0]
    got_marks_ref[0] = marks_ref[0]
    low_lane = lax.broadcasted_iota(jnp.int32, (1, LANES), 1) < ROOM

    def arrive(k):
        for a in range(FAN):
            if k + a > 0:
                marks_copy(me, FAN * k + a).wait_recv()
                sums_copy(me, FAN * k + a).wait_recv()
        for h in range(2):
            at = slice(k * TILE + h * LANES, k * TILE + (h + 1) * LANES)
            low = got_marks_ref[FAN * k + 2 * h]
            high = got_marks_ref[FAN * k + 2 * h + 1]
            name = jnp.where(low_lane, low[0:1, :], high[0:1, :])
            unit = jnp.where(low_lane, low[1:2, :], high[1:2, :])
            names_ref[:, at] = name
            gains_ref[:, at] = unit
            tags_ref[at, :] = jnp.broadcast_to(name, (LANES, LANES)).T
            factors_ref[at, :] = jnp.broadcast_to(unit, (LANES, LANES)).T
            where_ref[2 * k + h : 2 * k + h + 1, :] = jnp.where(name < 0.0, float(rows_dev), name).astype(jnp.int32)
        for a in range(FAN):
            code = got_ref[FAN * k + a].astype(jnp.int32).astype(jnp.float32)
            big = code.astype(jnp.bfloat16)
            at = slice(k * TILE + a * ROOM, k * TILE + (a + 1) * ROOM)
            split_ref[at, :LANES] = big
            split_ref[at, LANES:] = (code - big.astype(jnp.float32)).astype(jnp.bfloat16)

    def match(rows, first, last):
        tags = tags_ref[rows, :]
        hot = [
            jnp.where(tags == names_ref[:, at], gains_ref[:, at], 0.0).astype(jnp.bfloat16)
            for at in [slice(c * LANES, (c + 1) * LANES) for c in range(first * 2, last * 2)]
        ]
        hot = jnp.concatenate(hot, axis=1)
        out = jnp.dot(hot, split_ref[first * TILE : last * TILE, :], preferred_element_type=jnp.float32)
        return out[:, :LANES] + out[:, LANES:]

    def tile_rows(i):
        return pl.ds(pl.multiple_of(i * TILE, TILE), TILE)

    def fresh(i, last):
        all_ref[tile_rows(i), :] = match(tile_rows(i), 0, last)

    def more(i, first, last):
        all_ref[tile_rows(i), :] += match(tile_rows(i), first, last)

    def over(low, high, act):
        lax.fori_loop(low, high, lambda i, c: (act(i), c)[1], 0)

    done = 0
    for last in stages(groups):
        for k in range(done, last):
            arrive(k)
        if last < groups - 1:
            if done > 0:
                over(0, done, lambda i: more(i, done, last))
            over(done, last, lambda i: fresh(i, last))
        else:
            for i in range(done):
                more(i, done, last)
            for i in range(done, last):
                fresh(i, last)
        done = last

    squares = jnp.zeros((8, LANES), jnp.float32)
    for k in range(groups):
        for a in range(FAN):
            at = k * TILE + a * ROOM
            both = got_ref[FAN * k + a].astype(jnp.int32).astype(jnp.float32) * factors_ref[at : at + ROOM, :]
            both = both * all_ref[at : at + ROOM, :]
            squares = squares + jnp.sum(both.reshape(ROOM // 8, 8, LANES), axis=0)

    part_ref[...] = jnp.sum(squares, axis=0, keepdims=True)
    parts_ref[me] = part_ref[...]

    def part_copy(peer, source):
        return pltpu.make_async_remote_copy(
            src_ref=part_ref, dst_ref=parts_ref.at[source],
            send_sem=part_send.at[peer], recv_sem=part_recv.at[source],
            device_id={"dp": peer}, device_id_type=MESH,
        )

    def plane_copy(peer, source):
        return pltpu.make_async_remote_copy(
            src_ref=plane_ref, dst_ref=planes_ref.at[source],
            send_sem=plane_send.at[peer], recv_sem=plane_recv.at[source],
            device_id={"mp": peer}, device_id_type=MESH,
        )

    def each_peer(act):
        def one(step, carry):
            act(lax.rem(me + step, n))
            return carry

        lax.fori_loop(1, n, one, 0)

    each_peer(lambda peer: part_copy(peer, me).start())
    each_peer(lambda peer: part_copy(me, peer).wait_recv())
    plane_ref[...] = jnp.sum(parts_ref[...], axis=0)
    planes_ref[col] = plane_ref[...]
    for step in range(1, others):
        plane_copy(lax.rem(col + step, others), col).start()
    for step in range(1, others):
        plane_copy(col, lax.rem(col + step, others)).wait_recv()
    total_ref[...] = jnp.sum(planes_ref[...], axis=0)

    each_peer(lambda peer: part_copy(peer, me).wait_send())
    for place in range(1, n):
        marks_copy(me, place).wait_send()
        sums_copy(me, place).wait_send()
    for step in range(1, others):
        plane_copy(lax.rem(col + step, others), col).wait_send()


def update_kernel(
    limit, total_ref, where_hbm, all_ref, table_ref, first_ref, second_ref, new_table_hbm, new_first_hbm, new_second_hbm,
    where_ref, rows_ref, new_table_ref, new_first_ref, new_second_ref, where_sem, out_sem,
):
    load = pltpu.make_async_copy(where_hbm, where_ref, where_sem)
    load.start()
    rows_dev = table_ref.shape[0]
    chunk = 512

    def clear(i, carry):
        rows_ref[pl.ds(pl.multiple_of(i * chunk, chunk), chunk), :] = jnp.zeros((chunk, LANES), jnp.float32)
        return carry

    lax.fori_loop(0, rows_dev // chunk, clear, 0)
    total = jnp.sum(total_ref[...], axis=1, keepdims=True)
    scale = limit / jnp.maximum(jnp.sqrt(total), limit)
    load.wait()

    def place(i, carry):
        base = pl.multiple_of(i * LANES, LANES)
        for u in range(LANES):
            rows_ref[pl.ds(where_ref[i, u], 1), :] = all_ref[pl.ds(base + u, 1), :]
        return carry

    lax.fori_loop(0, all_ref.shape[0] // LANES, place, 0)

    def outs(i):
        at = pl.ds(pl.multiple_of(i * chunk, chunk), chunk)
        return [
            pltpu.make_async_copy(ref.at[at, :], hbm.at[at, :], out_sem.at[w, i])
            for w, (ref, hbm) in enumerate(
                [(new_table_ref, new_table_hbm), (new_first_ref, new_first_hbm), (new_second_ref, new_second_hbm)]
            )
        ]

    root = second_fix**0.5

    def update(i, carry):
        at = pl.ds(pl.multiple_of(i * chunk, chunk), chunk)
        clipped = scale * rows_ref[at, :]
        first = beta_first * first_ref[at, :] + (1.0 - beta_first) * clipped
        second = beta_second * second_ref[at, :] + (1.0 - beta_second) * clipped * clipped
        new_first_ref[at, :] = first
        new_second_ref[at, :] = second
        step = (learn_rate * root / first_fix) * first / (second * lax.rsqrt(second) + adam_eps * root)
        new_table_ref[at, :] = (1.0 - learn_rate * decay_rate) * table_ref[at, :] - step
        for copy in outs(i):
            copy.start()
        return carry

    lax.fori_loop(0, rows_dev // chunk, update, 0)

    def finish(i, carry):
        for copy in outs(i):
            copy.wait()
        return carry

    lax.fori_loop(0, rows_dev // chunk, finish, 0)


def body(table, first_moment, second_moment, grads, ids):
    n = lax.axis_size("dp")
    others = lax.axis_size("mp")
    rows_dev, width = table.shape
    tok_dev = grads.shape[0]
    slots = n * ROOM
    dma = pltpu.SemaphoreType.DMA
    vmem = pl.BlockSpec(memory_space=pltpu.VMEM)
    hbm = pl.BlockSpec(memory_space=pltpu.HBM)
    anywhere = pl.BlockSpec(memory_space=pl.ANY)
    sums, where, total = pl.pallas_call(
        functools.partial(exchange_kernel, n, others, rows_dev),
        out_shape=(
            jax.ShapeDtypeStruct((slots, width), jnp.float32),
            jax.ShapeDtypeStruct((slots // LANES, LANES), jnp.int32),
            jax.ShapeDtypeStruct((1, LANES), jnp.float32),
        ),
        in_specs=[hbm, hbm],
        out_specs=(vmem, vmem, vmem),
        scratch_shapes=[
            pltpu.VMEM((tok_dev // LANES, LANES), jnp.int32),
            pltpu.VMEM((tok_dev, LANES), jnp.int32),
            pltpu.VMEM((tok_dev, 2 * LANES), jnp.bfloat16),
            pltpu.VMEM((1, tok_dev), jnp.int32),
            pltpu.VMEM((1, tok_dev), jnp.int32),
            pltpu.VMEM((n, ROOM, width), jnp.int16),
            pltpu.VMEM((n // 2, 2, LANES), jnp.float32),
            pltpu.VMEM((n, ROOM, width), jnp.int16),
            pltpu.VMEM((n, 2, LANES), jnp.float32),
            pltpu.VMEM((slots, 2 * LANES), jnp.bfloat16),
            pltpu.VMEM((1, slots), jnp.float32),
            pltpu.VMEM((1, slots), jnp.float32),
            pltpu.VMEM((slots, LANES), jnp.float32),
            pltpu.VMEM((slots, LANES), jnp.float32),
            pltpu.VMEM((1, LANES), jnp.float32),
            pltpu.VMEM((n, 1, LANES), jnp.float32),
            pltpu.VMEM((1, LANES), jnp.float32),
            pltpu.VMEM((others, 1, LANES), jnp.float32),
            dma,
            dma,
            dma((n,)),
            dma((n,)),
            dma((n,)),
            dma((n,)),
            dma((n,)),
            dma((n,)),
            dma((others,)),
            dma((others,)),
        ],
        compiler_params=pltpu.CompilerParams(
            collective_id=0, has_side_effects=True, vmem_limit_bytes=20 * 1024 * 1024
        ),
        cost_estimate=pl.CostEstimate(flops=10**11, bytes_accessed=10**8, transcendentals=0),
    )(ids.reshape(tok_dev // LANES, LANES), grads)

    limit = float(tok_dev * n * width * others) ** 0.5
    shape = jax.ShapeDtypeStruct((rows_dev, width), jnp.float32)
    chunks = rows_dev // 512
    return pl.pallas_call(
        functools.partial(update_kernel, limit),
        out_shape=(shape, shape, shape),
        in_specs=[vmem, anywhere, vmem, vmem, vmem, vmem],
        out_specs=(hbm, hbm, hbm),
        scratch_shapes=[
            pltpu.SMEM((slots // LANES, LANES), jnp.int32),
            pltpu.VMEM((rows_dev + 8, width), jnp.float32),
            pltpu.VMEM((rows_dev, width), jnp.float32),
            pltpu.VMEM((rows_dev, width), jnp.float32),
            pltpu.VMEM((rows_dev, width), jnp.float32),
            dma,
            dma((3, chunks)),
        ],
        compiler_params=pltpu.CompilerParams(vmem_limit_bytes=40 * 1024 * 1024),
    )(total, where, sums, table, first_moment, second_moment)


def solution(mesh):
    placed = (P("dp", "mp"), P("dp", "mp"), P("dp", "mp"), P("dp", "mp"), P("dp"))
    return jax.shard_map(
        body,
        mesh=mesh,
        in_specs=placed,
        out_specs=(P("dp", "mp"), P("dp", "mp"), P("dp", "mp")),
        check_vma=False,
    )
```

```python
import functools

import jax
import jax.numpy as jnp
from jax import lax
from jax.experimental import pallas as pl
from jax.experimental.pallas import tpu as pltpu
from jax.sharding import PartitionSpec as P

beta_first = 0.9
beta_second = 0.999
learn_rate = 0.01
decay_rate = 0.1
adam_eps = 1e-08
first_fix = 0.9999734386
second_fix = 0.0952078529

LANES = 128
ROOM = 64
TILE = 256
FAN = TILE // ROOM
MESH = pl.DeviceIdType.MESH
BIG = 1 << 30
CODES = 32767.0


STEPS = [
    [(0, 0, 0), (0, 0, 1), (2, 2, 0), (2, 2, 1)],
    [(2, 1, 0), (1, 2, 0), (2, 3, 0), (3, 2, 0)],
    [(2, 1, 1), (1, 2, 1), (2, 3, 1), (3, 2, 1)],
    [(2, 0, 0), (0, 2, 0), (2, 0, 1), (0, 2, 1)],
    [(1, 1, 0), (3, 3, 0), (1, 3, 0), (3, 1, 0)],
    [(1, 1, 1), (3, 3, 1), (1, 3, 1), (3, 1, 1)],
    [(1, 0, 0), (3, 0, 0), (0, 1, 0), (0, 3, 0)],
    [(1, 0, 1), (3, 0, 1), (0, 1, 1), (0, 3, 1)],
]
SIDE = 4


def peer_of(me, offset):
    core = lax.rem(me, 2)
    z = lax.rem(me // 2, SIDE)
    y = me // (2 * SIDE)
    core = 1 - core if offset[2] else core
    return (lax.rem(y + offset[0], SIDE) * SIDE + lax.rem(z + offset[1], SIDE)) * 2 + core


def rank_tokens(ids_ref, spread_ref, joined_ref, owner_ref, slot_ref, rows_dev):
    blocks = ids_ref.shape[0]
    ids = ids_ref[...]
    columns = ids.T
    lane = lax.broadcasted_iota(jnp.int32, (LANES, LANES), 1)
    place = lax.broadcasted_iota(jnp.int32, (LANES, LANES), 0)
    shift = jnp.where(lane == 0, 6, 0)
    keep = jnp.where(lane == 0, rows_dev // 64 - 1, jnp.where(lane == 1, 63, 0))
    one = jnp.where(lane == 2, 1, 0)
    later = jnp.where(lane < place, 0.0, 1.0)
    for i in range(blocks):
        mine = jnp.broadcast_to(columns[:, i : i + 1], (LANES, LANES))
        marks = (lax.shift_right_logical(mine, shift) & keep) | one
        joined_ref[i * LANES : (i + 1) * LANES, LANES:] = marks.astype(jnp.float32).astype(jnp.bfloat16)
        alone = jnp.where(mine == ids[i : i + 1, :], later, 1.0)
        for j in range(i):
            alone = jnp.where(mine == ids[j : j + 1, :], 0.0, alone)
        least = jnp.min(alone, axis=1, keepdims=True)
        spread_ref[i * LANES : (i + 1) * LANES, :] = jnp.where(least > 0.0, mine, BIG)

    queries = [jnp.broadcast_to(ids[j : j + 1, :], (8, LANES)) for j in range(blocks)]
    queries.append(lax.broadcasted_iota(jnp.int32, (8, LANES), 1) * rows_dev)
    sums = []
    for part in (queries[:9], queries[9:]):

        def count(step, found, part=part):
            for u in range(8):
                other = spread_ref[pl.ds(pl.multiple_of(step * 64, 64) + 8 * u, 8), :]
                found = tuple(f + lax.shift_right_logical(other - q, 31) for f, q in zip(found, part))
            return found

        zero = jnp.zeros((8, LANES), jnp.int32)
        sums.extend(lax.fori_loop(0, blocks * LANES // 64, count, (zero,) * len(part)))
    below = [jnp.sum(s.astype(jnp.float32), axis=0, keepdims=True).astype(jnp.int32) for s in sums]
    start = jnp.broadcast_to(below[-1], (8, LANES))
    for j in range(blocks):
        owner = ids[j : j + 1, :] // rows_dev
        first = jnp.take_along_axis(start, jnp.broadcast_to(owner, (8, LANES)), axis=1)[0:1, :]
        owner_ref[:, j * LANES : (j + 1) * LANES] = owner
        slot_ref[:, j * LANES : (j + 1) * LANES] = below[j] - first


def exchange_kernel(
    n, others, rows_dev, ids_hbm, grads_ref, all_ref, where_ref, total_ref,
    ids_ref, spread_ref, joined_ref, owner_ref, slot_ref, sums_ref, marks_ref, got_ref, got_marks_ref, split_ref,
    names_ref, gains_ref, tags_ref, factors_ref,
    part_ref, parts_ref, plane_ref, planes_ref,
    load_sem, ids_sem, sums_send, sums_recv, marks_send, marks_recv, part_send, part_recv, plane_send, plane_recv,
):
    me = lax.axis_index("dp")
    col = lax.axis_index("mp")
    groups = n // FAN

    ids_load = pltpu.make_async_copy(ids_hbm, ids_ref, ids_sem)
    ids_load.start()
    load = pltpu.make_async_copy(grads_ref, joined_ref.at[:, 0:LANES], load_sem)
    load.start()
    barrier = pltpu.get_barrier_semaphore()

    def greet(step, carry):
        pl.semaphore_signal(barrier, inc=1, device_id={"dp": lax.rem(me + step, n)}, device_id_type=MESH)
        return carry

    lax.fori_loop(1, n, greet, 0)
    for step in range(1, others):
        pl.semaphore_signal(barrier, inc=1, device_id={"mp": lax.rem(col + step, others)}, device_id_type=MESH)

    ids_load.wait()
    rank_tokens(ids_ref, spread_ref, joined_ref, owner_ref, slot_ref, rows_dev)
    load.wait()

    def sums_copy(peer, place):
        return pltpu.make_async_remote_copy(
            src_ref=sums_ref.at[place], dst_ref=got_ref.at[place],
            send_sem=sums_send.at[place], recv_sem=sums_recv.at[place],
            device_id={"dp": peer}, device_id_type=MESH,
        )

    def marks_copy(peer, place):
        return pltpu.make_async_remote_copy(
            src_ref=marks_ref.at[place // 2], dst_ref=got_marks_ref.at[place],
            send_sem=marks_send.at[place], recv_sem=marks_recv.at[place],
            device_id={"dp": peer}, device_id_type=MESH,
        )

    tokens = owner_ref.shape[1]
    here = lax.broadcasted_iota(jnp.int32, (TILE, tokens), 0).astype(jnp.float32).astype(jnp.bfloat16)
    lane = lax.broadcasted_iota(jnp.int32, (LANES, LANES), 1)

    for k in range(groups):
        peers = [peer_of(me, offset) for offset in STEPS[k]]
        owner = owner_ref[...]
        slot = slot_ref[...]
        row = jnp.full_like(slot, -1)
        for a in range(FAN):
            row = jnp.where(owner == peers[a], slot + a * ROOM, row)
        row = row.astype(jnp.float32).astype(jnp.bfloat16)
        hot = jnp.where(here == row, jnp.bfloat16(1), jnp.bfloat16(0))
        out = jnp.dot(hot, joined_ref[...], preferred_element_type=jnp.float32)
        for h in range(2):
            value = out[h * LANES : (h + 1) * LANES, :LANES]
            most = jnp.max(jnp.abs(value), axis=1, keepdims=True)
            unit = jnp.maximum(most * ((1.0 + 2.0**-7) / CODES), 1e-30).astype(jnp.bfloat16).astype(jnp.float32)
            code = jnp.clip(jnp.round(value * (1.0 / unit)), -CODES, CODES).astype(jnp.int32).astype(jnp.int16)
            for a in range(2):
                sums_ref[FAN * k + 2 * h + a] = code[a * ROOM : (a + 1) * ROOM, :]
            turned = jnp.where(lane == 3, unit, out[h * LANES : (h + 1) * LANES, LANES:]).T
            times = turned[2:3, :]
            name = (turned[0:1, :] * 64.0 + turned[1:2, :]) / jnp.maximum(times, 1.0)
            marks_ref[2 * k + h, 0:1, :] = jnp.where(times > 0.0, jnp.floor(name + 0.5), -1.0)
            marks_ref[2 * k + h, 1:2, :] = turned[3:4, :]
        if k == 0:
            pl.semaphore_wait(barrier, n - 1 + others - 1)
        for a in range(FAN):
            if k + a > 0:
                marks_copy(peers[a], FAN * k + a).start()
                sums_copy(peers[a], FAN * k + a).start()

    got_ref[0] = sums_ref[0]
    got_marks_ref[0] = marks_ref[0]
    low_lane = lax.broadcasted_iota(jnp.int32, (1, LANES), 1) < ROOM

    def arrive(k):
        for a in range(FAN):
            if k + a > 0:
                marks_copy(me, FAN * k + a).wait_recv()
                sums_copy(me, FAN * k + a).wait_recv()
        for h in range(2):
            at = slice(k * TILE + h * LANES, k * TILE + (h + 1) * LANES)
            low = got_marks_ref[FAN * k + 2 * h]
            high = got_marks_ref[FAN * k + 2 * h + 1]
            name = jnp.where(low_lane, low[0:1, :], high[0:1, :])
            unit = jnp.where(low_lane, low[1:2, :], high[1:2, :])
            names_ref[:, at] = name
            gains_ref[:, at] = unit
            tags_ref[at, :] = jnp.broadcast_to(name, (LANES, LANES)).T
            factors_ref[at, :] = jnp.broadcast_to(unit, (LANES, LANES)).T
            where_ref[2 * k + h : 2 * k + h + 1, :] = jnp.where(name < 0.0, float(rows_dev), name).astype(jnp.int32)
        for a in range(FAN):
            code = got_ref[FAN * k + a].astype(jnp.int32).astype(jnp.float32)
            big = code.astype(jnp.bfloat16)
            at = slice(k * TILE + a * ROOM, k * TILE + (a + 1) * ROOM)
            split_ref[at, :LANES] = big
            split_ref[at, LANES:] = (code - big.astype(jnp.float32)).astype(jnp.bfloat16)

    def match(rows, first, last):
        tags = tags_ref[rows, :]
        hot = [
            jnp.where(tags == names_ref[:, at], gains_ref[:, at], 0.0).astype(jnp.bfloat16)
            for at in [slice(c * LANES, (c + 1) * LANES) for c in range(first * 2, last * 2)]
        ]
        hot = jnp.concatenate(hot, axis=1)
        out = jnp.dot(hot, split_ref[first * TILE : last * TILE, :], preferred_element_type=jnp.float32)
        return out[:, :LANES] + out[:, LANES:]

    squares = jnp.zeros((8, LANES), jnp.float32)
    done = 0
    for last in (groups * 5 // 8, groups):
        for k in range(done, last):
            arrive(k)
        for k in range(done, last):
            at = slice(k * TILE, (k + 1) * TILE)
            near = match(at, k, k + 1)
            far = match(at, 0, k) if k > 0 else jnp.zeros_like(near)
            all_ref[at, :] = near + far
            value = got_ref[FAN * k : FAN * (k + 1)].astype(jnp.int32).astype(jnp.float32).reshape(TILE, LANES)
            both = value * factors_ref[at, :] * (near + 2.0 * far)
            squares = squares + jnp.sum(both.reshape(TILE // 8, 8, LANES), axis=0)
        done = last

    part_ref[...] = jnp.sum(squares, axis=0, keepdims=True)
    parts_ref[me] = part_ref[...]

    def part_copy(peer, source):
        return pltpu.make_async_remote_copy(
            src_ref=part_ref, dst_ref=parts_ref.at[source],
            send_sem=part_send.at[peer], recv_sem=part_recv.at[source],
            device_id={"dp": peer}, device_id_type=MESH,
        )

    def plane_copy(peer, source):
        return pltpu.make_async_remote_copy(
            src_ref=plane_ref, dst_ref=planes_ref.at[source],
            send_sem=plane_send.at[peer], recv_sem=plane_recv.at[source],
            device_id={"mp": peer}, device_id_type=MESH,
        )

    def each_peer(act):
        def one(step, carry):
            act(lax.rem(me + step, n))
            return carry

        lax.fori_loop(1, n, one, 0)

    each_peer(lambda peer: part_copy(peer, me).start())
    for k in range(groups - 1):
        at = slice(k * TILE, (k + 1) * TILE)
        all_ref[at, :] = all_ref[at, :] + match(at, k + 1, groups)
    least = jnp.min(where_ref[0 : 2 * groups, :].astype(jnp.float32), axis=0, keepdims=True)
    where_ref[2 * groups : 2 * groups + 1, :] = jnp.minimum(least, pltpu.roll(least, ROOM, 1)).astype(jnp.int32)
    each_peer(lambda peer: part_copy(me, peer).wait_recv())
    plane_ref[...] = jnp.sum(parts_ref[...], axis=0)
    planes_ref[col] = plane_ref[...]
    for step in range(1, others):
        plane_copy(lax.rem(col + step, others), col).start()
    for step in range(1, others):
        plane_copy(col, lax.rem(col + step, others)).wait_recv()
    total_ref[...] = jnp.sum(planes_ref[...], axis=0)

    each_peer(lambda peer: part_copy(peer, me).wait_send())
    for place in range(1, n):
        marks_copy(me, place).wait_send()
        sums_copy(me, place).wait_send()
    for step in range(1, others):
        plane_copy(lax.rem(col + step, others), col).wait_send()


def update_kernel(
    limit, total_ref, where_hbm, all_ref, table_ref, first_ref, second_ref, new_table_hbm, new_first_hbm, new_second_hbm,
    where_ref, rows_ref, new_table_ref, new_first_ref, new_second_ref, where_sem, out_sem,
):
    load = pltpu.make_async_copy(where_hbm, where_ref, where_sem)
    load.start()
    rows_dev = table_ref.shape[0]
    chunk = 512

    def clear(i, carry):
        rows_ref[pl.ds(pl.multiple_of(i * chunk, chunk), chunk), :] = jnp.zeros((chunk, LANES), jnp.float32)
        return carry

    lax.fori_loop(0, rows_dev // chunk, clear, 0)
    total = jnp.sum(total_ref[...], axis=1, keepdims=True)
    scale = limit / jnp.maximum(jnp.sqrt(total), limit)
    load.wait()

    halves = all_ref.shape[0] // LANES

    def place(i):
        for r in range(halves):
            for h in range(2):
                row = where_ref[r, i + h * ROOM]
                rows_ref[pl.ds(row, 1), :] = all_ref[pl.ds(r * LANES + h * ROOM + i, 1), :]
        return i + 1

    def outs(i):
        at = pl.ds(pl.multiple_of(i * chunk, chunk), chunk)
        return [
            pltpu.make_async_copy(ref.at[at, :], hbm.at[at, :], out_sem.at[w, i])
            for w, (ref, hbm) in enumerate(
                [(new_table_ref, new_table_hbm), (new_first_ref, new_first_hbm), (new_second_ref, new_second_hbm)]
            )
        ]

    root = second_fix**0.5

    def update(i, placed):
        end = (i + 1) * chunk
        placed = lax.while_loop(
            lambda s: jnp.logical_and(s < ROOM, where_ref[halves, jnp.minimum(s, ROOM - 1)] < end), place, placed
        )
        at = pl.ds(pl.multiple_of(i * chunk, chunk), chunk)
        clipped = scale * rows_ref[at, :]
        first = beta_first * first_ref[at, :] + (1.0 - beta_first) * clipped
        second = beta_second * second_ref[at, :] + (1.0 - beta_second) * clipped * clipped
        new_first_ref[at, :] = first
        new_second_ref[at, :] = second
        step = (learn_rate * root / first_fix) * first / (second * lax.rsqrt(second) + adam_eps * root)
        new_table_ref[at, :] = (1.0 - learn_rate * decay_rate) * table_ref[at, :] - step
        for copy in outs(i):
            copy.start()
        return placed

    lax.fori_loop(0, rows_dev // chunk, update, 0)

    def finish(i, carry):
        for copy in outs(i):
            copy.wait()
        return carry

    lax.fori_loop(0, rows_dev // chunk, finish, 0)


def body(table, first_moment, second_moment, grads, ids):
    n = lax.axis_size("dp")
    others = lax.axis_size("mp")
    rows_dev, width = table.shape
    tok_dev = grads.shape[0]
    slots = n * ROOM
    dma = pltpu.SemaphoreType.DMA
    vmem = pl.BlockSpec(memory_space=pltpu.VMEM)
    hbm = pl.BlockSpec(memory_space=pltpu.HBM)
    anywhere = pl.BlockSpec(memory_space=pl.ANY)
    sums, where, total = pl.pallas_call(
        functools.partial(exchange_kernel, n, others, rows_dev),
        out_shape=(
            jax.ShapeDtypeStruct((slots, width), jnp.float32),
            jax.ShapeDtypeStruct((slots // LANES + 8, LANES), jnp.int32),
            jax.ShapeDtypeStruct((1, LANES), jnp.float32),
        ),
        in_specs=[hbm, hbm],
        out_specs=(vmem, vmem, vmem),
        scratch_shapes=[
            pltpu.VMEM((tok_dev // LANES, LANES), jnp.int32),
            pltpu.VMEM((tok_dev, LANES), jnp.int32),
            pltpu.VMEM((tok_dev, 2 * LANES), jnp.bfloat16),
            pltpu.VMEM((1, tok_dev), jnp.int32),
            pltpu.VMEM((1, tok_dev), jnp.int32),
            pltpu.VMEM((n, ROOM, width), jnp.int16),
            pltpu.VMEM((n // 2, 2, LANES), jnp.float32),
            pltpu.VMEM((n, ROOM, width), jnp.int16),
            pltpu.VMEM((n, 2, LANES), jnp.float32),
            pltpu.VMEM((slots, 2 * LANES), jnp.bfloat16),
            pltpu.VMEM((1, slots), jnp.float32),
            pltpu.VMEM((1, slots), jnp.float32),
            pltpu.VMEM((slots, LANES), jnp.float32),
            pltpu.VMEM((slots, LANES), jnp.float32),
            pltpu.VMEM((1, LANES), jnp.float32),
            pltpu.VMEM((n, 1, LANES), jnp.float32),
            pltpu.VMEM((1, LANES), jnp.float32),
            pltpu.VMEM((others, 1, LANES), jnp.float32),
            dma,
            dma,
            dma((n,)),
            dma((n,)),
            dma((n,)),
            dma((n,)),
            dma((n,)),
            dma((n,)),
            dma((others,)),
            dma((others,)),
        ],
        compiler_params=pltpu.CompilerParams(
            collective_id=0, has_side_effects=True, vmem_limit_bytes=20 * 1024 * 1024
        ),
        cost_estimate=pl.CostEstimate(flops=10**11, bytes_accessed=10**8, transcendentals=0),
    )(pltpu.with_memory_space_constraint(ids.reshape(tok_dev // LANES, LANES), pltpu.HBM), pltpu.with_memory_space_constraint(grads, pltpu.HBM))

    limit = float(tok_dev * n * width * others) ** 0.5
    shape = jax.ShapeDtypeStruct((rows_dev, width), jnp.float32)
    chunks = rows_dev // 512
    return pl.pallas_call(
        functools.partial(update_kernel, limit),
        out_shape=(shape, shape, shape),
        in_specs=[vmem, anywhere, vmem, vmem, vmem, vmem],
        out_specs=(hbm, hbm, hbm),
        scratch_shapes=[
            pltpu.SMEM((slots // LANES + 8, LANES), jnp.int32),
            pltpu.VMEM((rows_dev + 8, width), jnp.float32),
            pltpu.VMEM((rows_dev, width), jnp.float32),
            pltpu.VMEM((rows_dev, width), jnp.float32),
            pltpu.VMEM((rows_dev, width), jnp.float32),
            dma,
            dma((3, chunks)),
        ],
        compiler_params=pltpu.CompilerParams(vmem_limit_bytes=40 * 1024 * 1024),
    )(total, where, sums, table, first_moment, second_moment)


def solution(mesh):
    placed = (P("dp", "mp"), P("dp", "mp"), P("dp", "mp"), P("dp", "mp"), P("dp"))
    return jax.shard_map(
        body,
        mesh=mesh,
        in_specs=placed,
        out_specs=(P("dp", "mp"), P("dp", "mp"), P("dp", "mp")),
        check_vma=False,
    )
```

```python
import functools

import jax
import jax.numpy as jnp
from jax import lax
from jax.experimental import pallas as pl
from jax.experimental.pallas import tpu as pltpu
from jax.sharding import PartitionSpec as P

beta_first = 0.9
beta_second = 0.999
learn_rate = 0.01
decay_rate = 0.1
adam_eps = 1e-08
first_fix = 0.9999734386
second_fix = 0.0952078529

LANES = 128
ROOM = 64
TILE = 256
FAN = TILE // ROOM
MESH = pl.DeviceIdType.MESH
CODES = 32767.0


STEPS = [
    [(0, 0, 0), (0, 0, 1), (2, 2, 0), (2, 2, 1)],
    [(2, 1, 0), (1, 2, 0), (2, 3, 0), (3, 2, 0)],
    [(2, 1, 1), (1, 2, 1), (2, 3, 1), (3, 2, 1)],
    [(2, 0, 0), (0, 2, 0), (2, 0, 1), (0, 2, 1)],
    [(1, 1, 0), (3, 3, 0), (1, 3, 0), (3, 1, 0)],
    [(1, 1, 1), (3, 3, 1), (1, 3, 1), (3, 1, 1)],
    [(1, 0, 0), (3, 0, 0), (0, 1, 0), (0, 3, 0)],
    [(1, 0, 1), (3, 0, 1), (0, 1, 1), (0, 3, 1)],
]
SIDE = 4


def peer_of(me, offset):
    core = lax.rem(me, 2)
    z = lax.rem(me // 2, SIDE)
    y = me // (2 * SIDE)
    core = 1 - core if offset[2] else core
    return (lax.rem(y + offset[0], SIDE) * SIDE + lax.rem(z + offset[1], SIDE)) * 2 + core


def name_slots(ids_ref, spread_ref, lead_ref, planes_ref, slots_ref, slot_ids_ref, n, rows_dev):
    blocks = ids_ref.shape[0]
    ids = ids_ref[...]
    columns = ids.T
    lane = lax.broadcasted_iota(jnp.int32, (LANES, LANES), 1)
    place = lax.broadcasted_iota(jnp.int32, (LANES, LANES), 0)
    earlier = jnp.where(place < lane, 0.0, 1.0)
    group = 8
    for i in range(blocks):
        spread_ref[i * LANES : (i + 1) * LANES, :] = jnp.broadcast_to(columns[:, i : i + 1], (LANES, LANES))
    owners = lax.broadcasted_iota(jnp.int32, (n, LANES), 0)
    for j in range(blocks):
        mine = ids[j : j + 1, :]
        alone = [jnp.ones((group, LANES), jnp.float32)] * 2
        for v in range(j * LANES // group):
            other = spread_ref[v * group : (v + 1) * group, :]
            alone[v % 2] = jnp.where(other == mine, 0.0, alone[v % 2])
        for v in range(LANES // group):
            other = spread_ref[j * LANES + v * group : j * LANES + (v + 1) * group, :]
            seen = jnp.where(other == mine, earlier[v * group : (v + 1) * group, :], 1.0)
            alone[v % 2] = jnp.minimum(alone[v % 2], seen)
        lead = jnp.min(jnp.minimum(alone[0], alone[1]), axis=0, keepdims=True)
        lead = jnp.where(mine // rows_dev == owners, lead, 0.0)
        at = slice((j // 2) * n, (j // 2 + 1) * n)
        lead_ref[at, (j % 2) * LANES : (j % 2 + 1) * LANES] = lead.astype(jnp.bfloat16)
        local = mine & (rows_dev - 1)
        cols = slice(j * LANES, (j + 1) * LANES)
        planes_ref[0:n, cols] = (lead * (local >> 6).astype(jnp.float32)).astype(jnp.bfloat16)
        planes_ref[n : 2 * n, cols] = (lead * (local & 63).astype(jnp.float32)).astype(jnp.bfloat16)
        planes_ref[2 * n : 3 * n, cols] = lead.astype(jnp.bfloat16)

    wide = lax.broadcasted_iota(jnp.int32, (TILE, TILE), 1)
    tall = lax.broadcasted_iota(jnp.int32, (TILE, TILE), 0)
    before = jnp.where(tall < wide, 1.0, 0.0).astype(jnp.bfloat16)
    lead = lead_ref[...]
    ahead = jnp.dot(lead, before, preferred_element_type=jnp.float32)
    lead = lead.astype(jnp.float32)
    sizes = jnp.sum(lead, axis=1, keepdims=True)
    carry = jnp.zeros((n, 1), jnp.float32)
    seats = lax.broadcasted_iota(jnp.int32, (LANES, TILE), 0).astype(jnp.float32)
    for b in range(blocks // 2):
        at = slice(b * n, (b + 1) * n)
        slot = jnp.sum(lead[at, :] * (ahead[at, :] + carry), axis=0, keepdims=True)
        slots_ref[:, b * TILE : (b + 1) * TILE] = jnp.where(seats == slot, 1.0, 0.0).astype(jnp.bfloat16)
        carry = carry + sizes[at, :]
    held = lax.dot_general(
        planes_ref[...], slots_ref[...], (((1,), (1,)), ((), ())), preferred_element_type=jnp.float32
    )
    name = held[0:n, :] * 64.0 + held[n : 2 * n, :]
    slot_ids_ref[...] = jnp.where(held[2 * n : 3 * n, :] > 0.5, name.astype(jnp.int32) + owners * rows_dev, -1)


def exchange_kernel(
    n, others, rows_dev, ids_hbm, grads_ref, all_ref, where_ref, total_ref,
    ids_ref, spread_ref, loaded_ref, turned_ref, lead_ref, planes_ref, slots_ref, slot_ids_ref, sums_ref, marks_ref, got_ref, got_marks_ref, split_ref,
    names_ref, gains_ref, tags_ref, factors_ref,
    part_ref, parts_ref, plane_ref, across_ref,
    load_sem, ids_sem, sums_send, sums_recv, marks_send, marks_recv, part_send, part_recv, plane_send, plane_recv,
):
    me = lax.axis_index("dp")
    col = lax.axis_index("mp")
    groups = n // FAN

    ids_load = pltpu.make_async_copy(ids_hbm, ids_ref, ids_sem)
    ids_load.start()
    load = pltpu.make_async_copy(grads_ref, loaded_ref, load_sem)
    load.start()
    barrier = pltpu.get_barrier_semaphore()

    def greet(step, carry):
        pl.semaphore_signal(barrier, inc=1, device_id={"dp": lax.rem(me + step, n)}, device_id_type=MESH)
        return carry

    lax.fori_loop(1, n, greet, 0)
    for step in range(1, others):
        pl.semaphore_signal(barrier, inc=1, device_id={"mp": lax.rem(col + step, others)}, device_id_type=MESH)

    ids_load.wait()
    name_slots(ids_ref, spread_ref, lead_ref, planes_ref, slots_ref, slot_ids_ref, n, rows_dev)
    load.wait()
    tokens = loaded_ref.shape[0]
    for i in range(tokens // TILE):
        at = slice(i * TILE, (i + 1) * TILE)
        turned_ref[:, at] = loaded_ref[at, :].T

    def sums_copy(peer, place):
        return pltpu.make_async_remote_copy(
            src_ref=sums_ref.at[place], dst_ref=got_ref.at[place],
            send_sem=sums_send.at[place], recv_sem=sums_recv.at[place],
            device_id={"dp": peer}, device_id_type=MESH,
        )

    def marks_copy(peer, place):
        return pltpu.make_async_remote_copy(
            src_ref=marks_ref.at[place // 2], dst_ref=got_marks_ref.at[place],
            send_sem=marks_send.at[place], recv_sem=marks_recv.at[place],
            device_id={"dp": peer}, device_id_type=MESH,
        )

    low_lane = lax.broadcasted_iota(jnp.int32, (1, LANES), 1) < ROOM

    def pack(k):
        peers = [peer_of(me, offset) for offset in STEPS[k]]
        names = []
        hot = []
        for h in range(2):
            low = slot_ids_ref[pl.ds(peers[2 * h], 1), :]
            high = slot_ids_ref[pl.ds(peers[2 * h + 1], 1), :]
            names.append(jnp.where(low_lane, low, pltpu.roll(high, ROOM, 1)))
            hot.append(jnp.where(spread_ref[...] == names[h], 1.0, 0.0).astype(jnp.bfloat16))
        out = jnp.dot(turned_ref[...], jnp.concatenate(hot, axis=1), preferred_element_type=jnp.float32)
        return peers, names, out

    def keep(k, names, out):
        most = jnp.max(jnp.abs(out), axis=0, keepdims=True)
        unit = jnp.maximum(most * ((1.0 + 2.0**-7) / CODES), 1e-30).astype(jnp.bfloat16).astype(jnp.float32)
        code = jnp.clip(jnp.round(out * (1.0 / unit)), -CODES, CODES)
        for h in range(2):
            half = code[:, h * LANES : (h + 1) * LANES].T.astype(jnp.int32).astype(jnp.int16)
            for a in range(2):
                sums_ref[FAN * k + 2 * h + a] = half[a * ROOM : (a + 1) * ROOM, :]
            name = jnp.where(names[h] < 0, -1, names[h] & (rows_dev - 1))
            marks_ref[2 * k + h, 0:1, :] = name.astype(jnp.float32)
            marks_ref[2 * k + h, 1:2, :] = unit[:, h * LANES : (h + 1) * LANES]

    for k in range(0, groups, 2):
        both = [pack(k), pack(k + 1)]
        for u in range(2):
            keep(k + u, both[u][1], both[u][2])
        if k == 0:
            pl.semaphore_wait(barrier, n - 1 + others - 1)
        for u in range(2):
            for a in range(FAN):
                if k + u + a > 0:
                    marks_copy(both[u][0][a], FAN * (k + u) + a).start()
                    sums_copy(both[u][0][a], FAN * (k + u) + a).start()

    got_ref[0] = sums_ref[0]
    got_marks_ref[0] = marks_ref[0]
    def arrive(k):
        for a in range(FAN):
            if k + a > 0:
                marks_copy(me, FAN * k + a).wait_recv()
                sums_copy(me, FAN * k + a).wait_recv()
        for h in range(2):
            at = slice(k * TILE + h * LANES, k * TILE + (h + 1) * LANES)
            low = got_marks_ref[FAN * k + 2 * h]
            high = got_marks_ref[FAN * k + 2 * h + 1]
            name = jnp.where(low_lane, low[0:1, :], high[0:1, :])
            unit = jnp.where(low_lane, low[1:2, :], high[1:2, :])
            names_ref[:, at] = name
            gains_ref[:, at] = unit
            tags_ref[at, :] = jnp.broadcast_to(name, (LANES, LANES)).T
            factors_ref[at, :] = jnp.broadcast_to(unit, (LANES, LANES)).T
            where_ref[2 * k + h : 2 * k + h + 1, :] = jnp.where(name < 0.0, float(rows_dev), name).astype(jnp.int32)
        for a in range(FAN):
            code = got_ref[FAN * k + a].astype(jnp.int32).astype(jnp.float32)
            big = code.astype(jnp.bfloat16)
            at = slice(k * TILE + a * ROOM, k * TILE + (a + 1) * ROOM)
            split_ref[at, :LANES] = big
            split_ref[at, LANES:] = (code - big.astype(jnp.float32)).astype(jnp.bfloat16)

    def match(rows, first, last):
        tags = tags_ref[rows, :]
        hot = [
            jnp.where(tags == names_ref[:, at], gains_ref[:, at], 0.0).astype(jnp.bfloat16)
            for at in [slice(c * LANES, (c + 1) * LANES) for c in range(first * 2, last * 2)]
        ]
        hot = jnp.concatenate(hot, axis=1)
        out = jnp.dot(hot, split_ref[first * TILE : last * TILE, :], preferred_element_type=jnp.float32)
        return out[:, :LANES] + out[:, LANES:]

    squares = jnp.zeros((8, LANES), jnp.float32)
    done = 0
    for last in (groups * 5 // 8, groups):
        for k in range(done, last):
            arrive(k)
        for k in range(done, last):
            at = slice(k * TILE, (k + 1) * TILE)
            near = match(at, k, k + 1)
            far = match(at, 0, k) if k > 0 else jnp.zeros_like(near)
            all_ref[at, :] = near + far
            value = got_ref[FAN * k : FAN * (k + 1)].astype(jnp.int32).astype(jnp.float32).reshape(TILE, LANES)
            both = value * factors_ref[at, :] * (near + 2.0 * far)
            squares = squares + jnp.sum(both.reshape(TILE // 8, 8, LANES), axis=0)
        done = last

    part_ref[...] = jnp.sum(squares, axis=0, keepdims=True)
    parts_ref[me] = part_ref[...]

    def part_copy(peer, source):
        return pltpu.make_async_remote_copy(
            src_ref=part_ref, dst_ref=parts_ref.at[source],
            send_sem=part_send.at[peer], recv_sem=part_recv.at[source],
            device_id={"dp": peer}, device_id_type=MESH,
        )

    def plane_copy(peer, source):
        return pltpu.make_async_remote_copy(
            src_ref=plane_ref, dst_ref=across_ref.at[source],
            send_sem=plane_send.at[peer], recv_sem=plane_recv.at[source],
            device_id={"mp": peer}, device_id_type=MESH,
        )

    def each_peer(act):
        def one(step, carry):
            act(lax.rem(me + step, n))
            return carry

        lax.fori_loop(1, n, one, 0)

    each_peer(lambda peer: part_copy(peer, me).start())
    for k in range(groups - 1):
        at = slice(k * TILE, (k + 1) * TILE)
        all_ref[at, :] = all_ref[at, :] + match(at, k + 1, groups)
    each_peer(lambda peer: part_copy(me, peer).wait_recv())
    plane_ref[...] = jnp.sum(parts_ref[...], axis=0)
    across_ref[col] = plane_ref[...]
    for step in range(1, others):
        plane_copy(lax.rem(col + step, others), col).start()
    for step in range(1, others):
        plane_copy(col, lax.rem(col + step, others)).wait_recv()
    total_ref[...] = jnp.sum(across_ref[...], axis=0)

    each_peer(lambda peer: part_copy(peer, me).wait_send())
    for place in range(1, n):
        marks_copy(me, place).wait_send()
        sums_copy(me, place).wait_send()
    for step in range(1, others):
        plane_copy(lax.rem(col + step, others), col).wait_send()


def update_kernel(
    limit, total_ref, where_hbm, all_ref, table_ref, first_ref, second_ref, new_table_hbm, new_first_hbm, new_second_hbm,
    where_ref, rows_ref, new_table_ref, new_first_ref, new_second_ref, where_sem, out_sem,
):
    load = pltpu.make_async_copy(where_hbm, where_ref, where_sem)
    load.start()
    rows_dev = table_ref.shape[0]
    chunk = 512

    def clear(i, carry):
        rows_ref[pl.ds(pl.multiple_of(i * chunk, chunk), chunk), :] = jnp.zeros((chunk, LANES), jnp.float32)
        return carry

    lax.fori_loop(0, rows_dev // chunk, clear, 0)
    total = jnp.sum(total_ref[...], axis=1, keepdims=True)
    scale = limit / jnp.maximum(jnp.sqrt(total), limit)
    load.wait()

    halves = all_ref.shape[0] // LANES

    def place(i, carry):
        base = pl.multiple_of(i * LANES, LANES)
        for u in range(LANES):
            rows_ref[pl.ds(where_ref[i, u], 1), :] = all_ref[pl.ds(base + u, 1), :]
        return carry

    lax.fori_loop(0, all_ref.shape[0] // LANES, place, 0)

    def outs(i):
        at = pl.ds(pl.multiple_of(i * chunk, chunk), chunk)
        return [
            pltpu.make_async_copy(ref.at[at, :], hbm.at[at, :], out_sem.at[w, i])
            for w, (ref, hbm) in enumerate(
                [(new_table_ref, new_table_hbm), (new_first_ref, new_first_hbm), (new_second_ref, new_second_hbm)]
            )
        ]

    root = second_fix**0.5

    def update(i, carry):
        at = pl.ds(pl.multiple_of(i * chunk, chunk), chunk)
        clipped = scale * rows_ref[at, :]
        first = beta_first * first_ref[at, :] + (1.0 - beta_first) * clipped
        second = beta_second * second_ref[at, :] + (1.0 - beta_second) * clipped * clipped
        new_first_ref[at, :] = first
        new_second_ref[at, :] = second
        step = (learn_rate * root / first_fix) * first / (second * lax.rsqrt(second) + adam_eps * root)
        new_table_ref[at, :] = (1.0 - learn_rate * decay_rate) * table_ref[at, :] - step
        for copy in outs(i):
            copy.start()
        return carry

    lax.fori_loop(0, rows_dev // chunk, update, 0)

    def finish(i, carry):
        for copy in outs(i):
            copy.wait()
        return carry

    lax.fori_loop(0, rows_dev // chunk, finish, 0)


def body(table, first_moment, second_moment, grads, ids):
    n = lax.axis_size("dp")
    others = lax.axis_size("mp")
    rows_dev, width = table.shape
    tok_dev = grads.shape[0]
    slots = n * ROOM
    dma = pltpu.SemaphoreType.DMA
    vmem = pl.BlockSpec(memory_space=pltpu.VMEM)
    hbm = pl.BlockSpec(memory_space=pltpu.HBM)
    anywhere = pl.BlockSpec(memory_space=pl.ANY)
    sums, where, total = pl.pallas_call(
        functools.partial(exchange_kernel, n, others, rows_dev),
        out_shape=(
            jax.ShapeDtypeStruct((slots, width), jnp.float32),
            jax.ShapeDtypeStruct((slots // LANES, LANES), jnp.int32),
            jax.ShapeDtypeStruct((1, LANES), jnp.float32),
        ),
        in_specs=[hbm, hbm],
        out_specs=(vmem, vmem, vmem),
        scratch_shapes=[
            pltpu.VMEM((tok_dev // LANES, LANES), jnp.int32),
            pltpu.VMEM((tok_dev, LANES), jnp.int32),
            pltpu.VMEM((tok_dev, LANES), jnp.bfloat16),
            pltpu.VMEM((LANES, tok_dev), jnp.bfloat16),
            pltpu.VMEM((tok_dev // TILE * n, TILE), jnp.bfloat16),
            pltpu.VMEM((3 * n, tok_dev), jnp.bfloat16),
            pltpu.VMEM((LANES, tok_dev), jnp.bfloat16),
            pltpu.VMEM((n, LANES), jnp.int32),
            pltpu.VMEM((n, ROOM, width), jnp.int16),
            pltpu.VMEM((n // 2, 2, LANES), jnp.float32),
            pltpu.VMEM((n, ROOM, width), jnp.int16),
            pltpu.VMEM((n, 2, LANES), jnp.float32),
            pltpu.VMEM((slots, 2 * LANES), jnp.bfloat16),
            pltpu.VMEM((1, slots), jnp.float32),
            pltpu.VMEM((1, slots), jnp.float32),
            pltpu.VMEM((slots, LANES), jnp.float32),
            pltpu.VMEM((slots, LANES), jnp.float32),
            pltpu.VMEM((1, LANES), jnp.float32),
            pltpu.VMEM((n, 1, LANES), jnp.float32),
            pltpu.VMEM((1, LANES), jnp.float32),
            pltpu.VMEM((others, 1, LANES), jnp.float32),
            dma,
            dma,
            dma((n,)),
            dma((n,)),
            dma((n,)),
            dma((n,)),
            dma((n,)),
            dma((n,)),
            dma((others,)),
            dma((others,)),
        ],
        compiler_params=pltpu.CompilerParams(
            collective_id=0, has_side_effects=True, vmem_limit_bytes=20 * 1024 * 1024
        ),
        cost_estimate=pl.CostEstimate(flops=10**11, bytes_accessed=10**8, transcendentals=0),
    )(pltpu.with_memory_space_constraint(ids.reshape(tok_dev // LANES, LANES), pltpu.HBM), pltpu.with_memory_space_constraint(grads, pltpu.HBM))

    limit = float(tok_dev * n * width * others) ** 0.5
    shape = jax.ShapeDtypeStruct((rows_dev, width), jnp.float32)
    chunks = rows_dev // 512
    return pl.pallas_call(
        functools.partial(update_kernel, limit),
        out_shape=(shape, shape, shape),
        in_specs=[vmem, anywhere, vmem, vmem, vmem, vmem],
        out_specs=(hbm, hbm, hbm),
        scratch_shapes=[
            pltpu.SMEM((slots // LANES, LANES), jnp.int32),
            pltpu.VMEM((rows_dev + 8, width), jnp.float32),
            pltpu.VMEM((rows_dev, width), jnp.float32),
            pltpu.VMEM((rows_dev, width), jnp.float32),
            pltpu.VMEM((rows_dev, width), jnp.float32),
            dma,
            dma((3, chunks)),
        ],
        compiler_params=pltpu.CompilerParams(vmem_limit_bytes=40 * 1024 * 1024),
    )(total, where, sums, table, first_moment, second_moment)


def solution(mesh):
    placed = (P("dp", "mp"), P("dp", "mp"), P("dp", "mp"), P("dp", "mp"), P("dp"))
    return jax.shard_map(
        body,
        mesh=mesh,
        in_specs=placed,
        out_specs=(P("dp", "mp"), P("dp", "mp"), P("dp", "mp")),
        check_vma=False,
    )
```

```python
import functools

import jax
import jax.numpy as jnp
from jax import lax
from jax.experimental import pallas as pl
from jax.experimental.pallas import tpu as pltpu
from jax.sharding import PartitionSpec as P

beta_first = 0.9
beta_second = 0.999
learn_rate = 0.01
decay_rate = 0.1
adam_eps = 1e-08
first_fix = 0.9999734386
second_fix = 0.0952078529

LANES = 128
ROOM = 64
TILE = 256
FAN = TILE // ROOM
MESH = pl.DeviceIdType.MESH
CODES = 32767.0


STEPS = [
    [(0, 0, 0), (0, 0, 1), (2, 2, 0), (2, 2, 1)],
    [(2, 1, 0), (1, 2, 0), (2, 3, 0), (3, 2, 0)],
    [(2, 1, 1), (1, 2, 1), (2, 3, 1), (3, 2, 1)],
    [(2, 0, 0), (0, 2, 0), (2, 0, 1), (0, 2, 1)],
    [(1, 1, 0), (3, 3, 0), (1, 3, 0), (3, 1, 0)],
    [(1, 1, 1), (3, 3, 1), (1, 3, 1), (3, 1, 1)],
    [(1, 0, 0), (3, 0, 0), (0, 1, 0), (0, 3, 0)],
    [(1, 0, 1), (3, 0, 1), (0, 1, 1), (0, 3, 1)],
]
SIDE = 4


def far_first():
    hops = [0, 1, 2, 1]
    away = [offset for step in STEPS for offset in step if any(offset)]
    return sorted(away, key=lambda offset: -(hops[offset[0]] + hops[offset[1]]))


def peer_of(me, offset):
    core = lax.rem(me, 2)
    z = lax.rem(me // 2, SIDE)
    y = me // (2 * SIDE)
    core = 1 - core if offset[2] else core
    return (lax.rem(y + offset[0], SIDE) * SIDE + lax.rem(z + offset[1], SIDE)) * 2 + core


def name_slots(ids_ref, spread_ref, lead_ref, planes_ref, slots_ref, slot_ids_ref, n, rows_dev):
    blocks = ids_ref.shape[0]
    ids = ids_ref[...]
    columns = ids.T
    lane = lax.broadcasted_iota(jnp.int32, (LANES, LANES), 1)
    place = lax.broadcasted_iota(jnp.int32, (LANES, LANES), 0)
    earlier = jnp.where(place < lane, 0.0, 1.0)
    group = 8
    for i in range(blocks):
        spread_ref[i * LANES : (i + 1) * LANES, :] = jnp.broadcast_to(columns[:, i : i + 1], (LANES, LANES))
    owners = lax.broadcasted_iota(jnp.int32, (n, LANES), 0)
    for j in range(blocks):
        mine = ids[j : j + 1, :]
        alone = [jnp.ones((group, LANES), jnp.float32)] * 2
        for v in range(j * LANES // group):
            other = spread_ref[v * group : (v + 1) * group, :]
            alone[v % 2] = jnp.where(other == mine, 0.0, alone[v % 2])
        for v in range(LANES // group):
            other = spread_ref[j * LANES + v * group : j * LANES + (v + 1) * group, :]
            seen = jnp.where(other == mine, earlier[v * group : (v + 1) * group, :], 1.0)
            alone[v % 2] = jnp.minimum(alone[v % 2], seen)
        lead = jnp.min(jnp.minimum(alone[0], alone[1]), axis=0, keepdims=True)
        lead = jnp.where(mine // rows_dev == owners, lead, 0.0)
        at = slice((j // 2) * n, (j // 2 + 1) * n)
        lead_ref[at, (j % 2) * LANES : (j % 2 + 1) * LANES] = lead.astype(jnp.bfloat16)
        local = mine & (rows_dev - 1)
        cols = slice(j * LANES, (j + 1) * LANES)
        planes_ref[0:n, cols] = (lead * (local >> 6).astype(jnp.float32)).astype(jnp.bfloat16)
        planes_ref[n : 2 * n, cols] = (lead * (local & 63).astype(jnp.float32)).astype(jnp.bfloat16)
        planes_ref[2 * n : 3 * n, cols] = lead.astype(jnp.bfloat16)

    wide = lax.broadcasted_iota(jnp.int32, (TILE, TILE), 1)
    tall = lax.broadcasted_iota(jnp.int32, (TILE, TILE), 0)
    before = jnp.where(tall < wide, 1.0, 0.0).astype(jnp.bfloat16)
    lead = lead_ref[...]
    ahead = jnp.dot(lead, before, preferred_element_type=jnp.float32)
    lead = lead.astype(jnp.float32)
    sizes = jnp.sum(lead, axis=1, keepdims=True)
    carry = jnp.zeros((n, 1), jnp.float32)
    seats = lax.broadcasted_iota(jnp.int32, (LANES, TILE), 0).astype(jnp.float32)
    for b in range(blocks // 2):
        at = slice(b * n, (b + 1) * n)
        slot = jnp.sum(lead[at, :] * (ahead[at, :] + carry), axis=0, keepdims=True)
        slots_ref[:, b * TILE : (b + 1) * TILE] = jnp.where(seats == slot, 1.0, 0.0).astype(jnp.bfloat16)
        carry = carry + sizes[at, :]
    held = lax.dot_general(
        planes_ref[...], slots_ref[...], (((1,), (1,)), ((), ())), preferred_element_type=jnp.float32
    )
    name = held[0:n, :] * 64.0 + held[n : 2 * n, :]
    name = jnp.where(held[2 * n : 3 * n, :] > 0.5, name, float(rows_dev)).astype(jnp.int32)
    seat = lax.broadcasted_iota(jnp.int32, (n, LANES), 1)
    name = jnp.where(seat < ROOM, name, pltpu.roll(name, ROOM, 1))
    rank = jnp.zeros((n, LANES), jnp.int32)
    for r in range(1, ROOM):
        rank = rank + lax.shift_right_logical(pltpu.roll(name, r, 1) - name, 31)
    both = name * ROOM + rank
    ordered = jnp.where(rank == seat, name, rows_dev)
    for r in range(1, ROOM):
        moved = pltpu.roll(both, r, 1)
        ordered = jnp.where((moved & (ROOM - 1)) == seat, moved >> 6, ordered)
    slot_ids_ref[...] = jnp.where(ordered < rows_dev, ordered + owners * rows_dev, -1)


def exchange_kernel(
    n, others, rows_dev, ids_hbm, grads_ref, all_ref, where_ref, total_ref,
    ids_ref, spread_ref, loaded_ref, turned_ref, lead_ref, planes_ref, slots_ref, slot_ids_ref, sums_ref, marks_ref, got_ref, got_marks_ref, split_ref,
    names_ref, gains_ref, tags_ref, factors_ref,
    part_ref, parts_ref, plane_ref, across_ref,
    load_sem, ids_sem, sums_send, sums_recv, marks_send, marks_recv, part_send, part_recv, plane_send, plane_recv,
):
    me = lax.axis_index("dp")
    col = lax.axis_index("mp")
    groups = n // FAN

    ids_load = pltpu.make_async_copy(ids_hbm, ids_ref, ids_sem)
    ids_load.start()
    load = pltpu.make_async_copy(grads_ref, loaded_ref, load_sem)
    load.start()
    barrier = pltpu.get_barrier_semaphore()

    def greet(step, carry):
        pl.semaphore_signal(barrier, inc=1, device_id={"dp": lax.rem(me + step, n)}, device_id_type=MESH)
        return carry

    lax.fori_loop(1, n, greet, 0)
    for step in range(1, others):
        pl.semaphore_signal(barrier, inc=1, device_id={"mp": lax.rem(col + step, others)}, device_id_type=MESH)

    ids_load.wait()
    name_slots(ids_ref, spread_ref, lead_ref, planes_ref, slots_ref, slot_ids_ref, n, rows_dev)
    load.wait()
    tokens = loaded_ref.shape[0]
    for i in range(tokens // TILE):
        at = slice(i * TILE, (i + 1) * TILE)
        turned_ref[:, at] = loaded_ref[at, :].T

    def sums_copy(peer, place):
        return pltpu.make_async_remote_copy(
            src_ref=sums_ref.at[place], dst_ref=got_ref.at[place],
            send_sem=sums_send.at[place], recv_sem=sums_recv.at[place],
            device_id={"dp": peer}, device_id_type=MESH,
        )

    def marks_copy(peer, place):
        return pltpu.make_async_remote_copy(
            src_ref=marks_ref.at[place // 2], dst_ref=got_marks_ref.at[place],
            send_sem=marks_send.at[place], recv_sem=marks_recv.at[place],
            device_id={"dp": peer}, device_id_type=MESH,
        )

    low_lane = lax.broadcasted_iota(jnp.int32, (1, LANES), 1) < ROOM

    def pack(k):
        peers = [peer_of(me, offset) for offset in STEPS[k]]
        names = []
        hot = []
        for h in range(2):
            low = slot_ids_ref[pl.ds(peers[2 * h], 1), :]
            high = slot_ids_ref[pl.ds(peers[2 * h + 1], 1), :]
            names.append(jnp.where(low_lane, low, pltpu.roll(high, ROOM, 1)))
            hot.append(jnp.where(spread_ref[...] == names[h], 1.0, 0.0).astype(jnp.bfloat16))
        out = jnp.dot(turned_ref[...], jnp.concatenate(hot, axis=1), preferred_element_type=jnp.float32)
        return peers, names, out

    def keep(k, names, out):
        most = jnp.max(jnp.abs(out), axis=0, keepdims=True)
        unit = jnp.maximum(most * ((1.0 + 2.0**-7) / CODES), 1e-30).astype(jnp.bfloat16).astype(jnp.float32)
        code = jnp.clip(jnp.round(out * (1.0 / unit)), -CODES, CODES)
        for h in range(2):
            half = code[:, h * LANES : (h + 1) * LANES].T.astype(jnp.int32).astype(jnp.int16)
            for a in range(2):
                sums_ref[FAN * k + 2 * h + a] = half[a * ROOM : (a + 1) * ROOM, :]
            name = jnp.where(names[h] < 0, -1, names[h] & (rows_dev - 1))
            marks_ref[2 * k + h, 0:1, :] = name.astype(jnp.float32)
            marks_ref[2 * k + h, 1:2, :] = unit[:, h * LANES : (h + 1) * LANES]

    for k in range(0, groups, 2):
        both = [pack(k), pack(k + 1)]
        for u in range(2):
            keep(k + u, both[u][1], both[u][2])
        if k == 0:
            pl.semaphore_wait(barrier, n - 1 + others - 1)
        for u in range(2):
            for a in range(FAN):
                if k + u + a > 0:
                    marks_copy(both[u][0][a], FAN * (k + u) + a).start()
                    sums_copy(both[u][0][a], FAN * (k + u) + a).start()

    got_ref[0] = sums_ref[0]
    got_marks_ref[0] = marks_ref[0]
    def arrive(k):
        for a in range(FAN):
            if k + a > 0:
                marks_copy(me, FAN * k + a).wait_recv()
                sums_copy(me, FAN * k + a).wait_recv()
        for h in range(2):
            at = slice(k * TILE + h * LANES, k * TILE + (h + 1) * LANES)
            low = got_marks_ref[FAN * k + 2 * h]
            high = got_marks_ref[FAN * k + 2 * h + 1]
            name = jnp.where(low_lane, low[0:1, :], high[0:1, :])
            unit = jnp.where(low_lane, low[1:2, :], high[1:2, :])
            names_ref[:, at] = name
            gains_ref[:, at] = unit
            tags_ref[at, :] = jnp.broadcast_to(name, (LANES, LANES)).T
            factors_ref[at, :] = jnp.broadcast_to(unit, (LANES, LANES)).T
            where_ref[2 * k + h : 2 * k + h + 1, :] = jnp.where(name < 0.0, float(rows_dev), name).astype(jnp.int32)
        for a in range(FAN):
            code = got_ref[FAN * k + a].astype(jnp.int32).astype(jnp.float32)
            big = code.astype(jnp.bfloat16)
            at = slice(k * TILE + a * ROOM, k * TILE + (a + 1) * ROOM)
            split_ref[at, :LANES] = big
            split_ref[at, LANES:] = (code - big.astype(jnp.float32)).astype(jnp.bfloat16)

    def match(rows, first, last):
        tags = tags_ref[rows, :]
        hot = [
            jnp.where(tags == names_ref[:, at], gains_ref[:, at], 0.0).astype(jnp.bfloat16)
            for at in [slice(c * LANES, (c + 1) * LANES) for c in range(first * 2, last * 2)]
        ]
        hot = jnp.concatenate(hot, axis=1)
        out = jnp.dot(hot, split_ref[first * TILE : last * TILE, :], preferred_element_type=jnp.float32)
        return out[:, :LANES] + out[:, LANES:]

    squares = jnp.zeros((8, LANES), jnp.float32)
    done = 0
    for last in (groups // 2, groups * 3 // 4, groups):
        for k in range(done, last):
            arrive(k)
        for k in range(done, last):
            at = slice(k * TILE, (k + 1) * TILE)
            near = match(at, k, k + 1)
            far = match(at, 0, k) if k > 0 else jnp.zeros_like(near)
            all_ref[at, :] = near + far
            value = got_ref[FAN * k : FAN * (k + 1)].astype(jnp.int32).astype(jnp.float32).reshape(TILE, LANES)
            both = value * factors_ref[at, :] * (near + 2.0 * far)
            squares = squares + jnp.sum(both.reshape(TILE // 8, 8, LANES), axis=0)
        done = last

    part_ref[...] = jnp.sum(squares, axis=0, keepdims=True)
    parts_ref[me] = part_ref[...]

    def part_copy(peer, source):
        return pltpu.make_async_remote_copy(
            src_ref=part_ref, dst_ref=parts_ref.at[source],
            send_sem=part_send.at[peer], recv_sem=part_recv.at[source],
            device_id={"dp": peer}, device_id_type=MESH,
        )

    def plane_copy(peer, source):
        return pltpu.make_async_remote_copy(
            src_ref=plane_ref, dst_ref=across_ref.at[source],
            send_sem=plane_send.at[peer], recv_sem=plane_recv.at[source],
            device_id={"mp": peer}, device_id_type=MESH,
        )

    def each_peer(act):
        def one(step, carry):
            act(lax.rem(me + step, n))
            return carry

        lax.fori_loop(1, n, one, 0)

    for offset in far_first():
        part_copy(peer_of(me, offset), me).start()
    for k in range(groups - 1):
        at = slice(k * TILE, (k + 1) * TILE)
        all_ref[at, :] = all_ref[at, :] + match(at, k + 1, groups)
    least = jnp.min(where_ref[0 : 2 * groups, :].astype(jnp.float32), axis=0, keepdims=True)
    where_ref[2 * groups : 2 * groups + 1, :] = jnp.minimum(least, pltpu.roll(least, ROOM, 1)).astype(jnp.int32)
    each_peer(lambda peer: part_copy(me, peer).wait_recv())
    plane_ref[...] = jnp.sum(parts_ref[...], axis=0)
    across_ref[col] = plane_ref[...]
    for step in range(1, others):
        plane_copy(lax.rem(col + step, others), col).start()
    for step in range(1, others):
        plane_copy(col, lax.rem(col + step, others)).wait_recv()
    total_ref[...] = jnp.sum(across_ref[...], axis=0)

    each_peer(lambda peer: part_copy(peer, me).wait_send())
    for place in range(1, n):
        marks_copy(me, place).wait_send()
        sums_copy(me, place).wait_send()
    for step in range(1, others):
        plane_copy(lax.rem(col + step, others), col).wait_send()


def update_kernel(
    limit, total_ref, where_hbm, all_ref, table_ref, first_ref, second_ref, new_table_hbm, new_first_hbm, new_second_hbm,
    where_ref, rows_ref, new_table_ref, new_first_ref, new_second_ref, where_sem, out_sem,
):
    load = pltpu.make_async_copy(where_hbm, where_ref, where_sem)
    load.start()
    rows_dev = table_ref.shape[0]
    chunk = 512

    def clear(i, carry):
        rows_ref[pl.ds(pl.multiple_of(i * chunk, chunk), chunk), :] = jnp.zeros((chunk, LANES), jnp.float32)
        return carry

    lax.fori_loop(0, rows_dev // chunk, clear, 0)
    total = jnp.sum(total_ref[...], axis=1, keepdims=True)
    scale = limit / jnp.maximum(jnp.sqrt(total), limit)
    load.wait()

    halves = all_ref.shape[0] // LANES

    halves = all_ref.shape[0] // LANES
    burst = 4

    def place(i):
        for r in range(halves):
            for h in range(2):
                for u in range(burst):
                    row = where_ref[i + (r * LANES + h * ROOM + u)]
                    rows_ref[pl.ds(row, 1), :] = all_ref[pl.ds(i + (r * LANES + h * ROOM + u), 1), :]
        return i + burst

    def outs(i):
        at = pl.ds(pl.multiple_of(i * chunk, chunk), chunk)
        return [
            pltpu.make_async_copy(ref.at[at, :], hbm.at[at, :], out_sem.at[w, i])
            for w, (ref, hbm) in enumerate(
                [(new_table_ref, new_table_hbm), (new_first_ref, new_first_hbm), (new_second_ref, new_second_hbm)]
            )
        ]

    first_gain = (1.0 - beta_first) * scale
    second_gain = (1.0 - beta_second) * scale * scale
    root = second_fix**0.5

    def update(i, placed):
        end = (i + 1) * chunk
        placed = lax.while_loop(
            lambda s: jnp.logical_and(s < ROOM, where_ref[halves * LANES + jnp.minimum(s, ROOM - 1)] < end), place, placed
        )
        at = pl.ds(pl.multiple_of(i * chunk, chunk), chunk)
        grad = rows_ref[at, :]
        first = beta_first * first_ref[at, :] + first_gain * grad
        second = beta_second * second_ref[at, :] + second_gain * (grad * grad)
        new_first_ref[at, :] = first
        new_second_ref[at, :] = second
        step = (learn_rate * root / first_fix) * first / (second * lax.rsqrt(second) + adam_eps * root)
        new_table_ref[at, :] = (1.0 - learn_rate * decay_rate) * table_ref[at, :] - step
        for copy in outs(i):
            copy.start()
        return placed

    lax.fori_loop(0, rows_dev // chunk, update, 0)

    def finish(i, carry):
        for copy in outs(i):
            copy.wait()
        return carry

    lax.fori_loop(0, rows_dev // chunk, finish, 0)


def body(table, first_moment, second_moment, grads, ids):
    n = lax.axis_size("dp")
    others = lax.axis_size("mp")
    rows_dev, width = table.shape
    tok_dev = grads.shape[0]
    slots = n * ROOM
    dma = pltpu.SemaphoreType.DMA
    vmem = pl.BlockSpec(memory_space=pltpu.VMEM)
    hbm = pl.BlockSpec(memory_space=pltpu.HBM)
    anywhere = pl.BlockSpec(memory_space=pl.ANY)
    sums, where, total = pl.pallas_call(
        functools.partial(exchange_kernel, n, others, rows_dev),
        out_shape=(
            jax.ShapeDtypeStruct((slots, width), jnp.float32),
            jax.ShapeDtypeStruct((slots // LANES + 8, LANES), jnp.int32),
            jax.ShapeDtypeStruct((1, LANES), jnp.float32),
        ),
        in_specs=[hbm, hbm],
        out_specs=(vmem, vmem, vmem),
        scratch_shapes=[
            pltpu.VMEM((tok_dev // LANES, LANES), jnp.int32),
            pltpu.VMEM((tok_dev, LANES), jnp.int32),
            pltpu.VMEM((tok_dev, LANES), jnp.bfloat16),
            pltpu.VMEM((LANES, tok_dev), jnp.bfloat16),
            pltpu.VMEM((tok_dev // TILE * n, TILE), jnp.bfloat16),
            pltpu.VMEM((3 * n, tok_dev), jnp.bfloat16),
            pltpu.VMEM((LANES, tok_dev), jnp.bfloat16),
            pltpu.VMEM((n, LANES), jnp.int32),
            pltpu.VMEM((n, ROOM, width), jnp.int16),
            pltpu.VMEM((n // 2, 2, LANES), jnp.float32),
            pltpu.VMEM((n, ROOM, width), jnp.int16),
            pltpu.VMEM((n, 2, LANES), jnp.float32),
            pltpu.VMEM((slots, 2 * LANES), jnp.bfloat16),
            pltpu.VMEM((1, slots), jnp.float32),
            pltpu.VMEM((1, slots), jnp.float32),
            pltpu.VMEM((slots, LANES), jnp.float32),
            pltpu.VMEM((slots, LANES), jnp.float32),
            pltpu.VMEM((1, LANES), jnp.float32),
            pltpu.VMEM((n, 1, LANES), jnp.float32),
            pltpu.VMEM((1, LANES), jnp.float32),
            pltpu.VMEM((others, 1, LANES), jnp.float32),
            dma,
            dma,
            dma((n,)),
            dma((n,)),
            dma((n,)),
            dma((n,)),
            dma((n,)),
            dma((n,)),
            dma((others,)),
            dma((others,)),
        ],
        compiler_params=pltpu.CompilerParams(
            collective_id=0, has_side_effects=True, vmem_limit_bytes=20 * 1024 * 1024
        ),
        cost_estimate=pl.CostEstimate(flops=10**11, bytes_accessed=10**8, transcendentals=0),
    )(pltpu.with_memory_space_constraint(ids.reshape(tok_dev // LANES, LANES), pltpu.HBM), pltpu.with_memory_space_constraint(grads, pltpu.HBM))

    limit = float(tok_dev * n * width * others) ** 0.5
    shape = jax.ShapeDtypeStruct((rows_dev, width), jnp.float32)
    chunks = rows_dev // 512
    return pl.pallas_call(
        functools.partial(update_kernel, limit),
        out_shape=(shape, shape, shape),
        in_specs=[vmem, anywhere, vmem, vmem, vmem, vmem],
        out_specs=(hbm, hbm, hbm),
        scratch_shapes=[
            pltpu.SMEM((slots + 8 * LANES,), jnp.int32),
            pltpu.VMEM((rows_dev + 8, width), jnp.float32),
            pltpu.VMEM((rows_dev, width), jnp.float32),
            pltpu.VMEM((rows_dev, width), jnp.float32),
            pltpu.VMEM((rows_dev, width), jnp.float32),
            dma,
            dma((3, chunks)),
        ],
        compiler_params=pltpu.CompilerParams(vmem_limit_bytes=40 * 1024 * 1024),
    )(total, where.reshape(slots + 8 * LANES), sums, table, first_moment, second_moment)


def solution(mesh):
    placed = (P("dp", "mp"), P("dp", "mp"), P("dp", "mp"), P("dp", "mp"), P("dp"))
    return jax.shard_map(
        body,
        mesh=mesh,
        in_specs=placed,
        out_specs=(P("dp", "mp"), P("dp", "mp"), P("dp", "mp")),
        check_vma=False,
    )
```
